32 devices in a mesh: groups: 2 (over y), seq: 4 (over z), beam: 4 (over x, core).
Axes of the slice: x: 2, y: 2, z: 4, core: 2. Of those that a mesh axis runs over, the one named last changes fastest.
Arguments:
- prompt_values: bfloat16 [2048, 8192], P(('groups', 'seq'), 'beam'), parts along dimension 0, may hold values from -6 to 6
- prompt_keys: bfloat16 [2048, 128], P(('groups', 'seq')), parts along dimension 0, may hold values from -0.31445312 to 0.31445312
- prompt_queries: bfloat16 [2048, 128], P(('groups', 'seq')), parts along dimension 0, may hold values from -0.31445312 to 0.31445312
- logarithm_state_decay: float32 [2048, 128], P(('groups', 'seq'), 'beam'), parts along dimension 0, may hold values from -1 to 0
- step_values: bfloat16 [8, 4, 8192], P('groups', 'beam', 'seq'), parts along dimension 0, may hold values from -6 to 6
- step_keys: bfloat16 [8, 4, 128], P('groups', 'beam'), parts along dimension 0, may hold values from -6 to 6
- step_queries: bfloat16 [8, 4, 128], P('groups', 'beam'), parts along dimension 0, may hold values from -0.31445312 to 0.31445312
- step_decay: float32 [8, 4, 128], P('groups', 'beam', 'seq'), parts along dimension 0, may hold values from -0.6 to -0.02
- step_logprob: float32 [8, 4], P('groups', 'beam'), parts along dimension 0, may hold values from -6 to -0.05
- parents: int32 [8, 4], P('groups', 'beam'), parts along dimension 0, may hold values from 0 to 3
- finished: int32 [8, 4], P('groups', 'beam'), parts along dimension 0, may hold values 0 or 1
- lengths: int32 [8], P(('groups', 'beam')), parts along dimension 0, may hold values from 1 to 59
- init_score: float32 [8], P(('groups', 'beam')), parts along dimension 0, may hold values from -20 to -2
Outputs:
- prompt_output: bfloat16 [2048, 8192], P(('groups', 'seq'), 'beam'), parts along dimension 0
- step_output: bfloat16 [8, 4, 8192], P('groups', 'beam', 'seq'), parts along dimension 0
- ranked: float32 [8, 4], P('groups', 'beam'), parts along dimension 0
- beam_states: float32 [8, 8192, 128], P(('groups', 'beam'), 'seq'), parts along dimension 0
The draws below stay inside these ranges and needn't reach their ends.
There are 2 independent parts, one for each index of `groups`. The reference program is written for one: setup_inputs(seed, part) draws one part's arguments, and reference() takes and returns one part's arrays. A program takes and returns all parts, laid end to end along the dimension named above; each array names one. Nothing has to cross between parts.
All inputs are finite; a program needn't handle non-finite values. No bound on the sum of `finished` on one device may be relied on, other than what follows from the above.
Results may differ from the reference program's by a relative error of at most 0.0056.
Values sent between devices are 32-bit elements; how exact they have to be, the bound alone decides.
No kernel may reach another device: no remote copies, remote signals or barrier semaphores. Data moves between devices by JAX's collectives and lax.ppermute only.
A program may use at most 64 MiB of HBM per device.

```python
import math
import jax
import jax.numpy as jnp
from jax import lax

H = 128
P_SIZE = 64
N = 128
STEPS = 4
TOK_DEV = 256
SPAN = 256
TOKENS = 1024
BEAMS = 4


def draw_logarithm_state_decay(key, part):
    keys = jax.random.split(jax.random.fold_in(key, 11), 7)
    slow_share = 0.5
    slow = jax.random.uniform(keys[0], (H,)) < slow_share
    slow_rate = jnp.exp(jax.random.uniform(keys[1], (H,), minval=math.log(0.05 / TOKENS), maxval=math.log(0.5 / TOKENS)))
    fast_rate = jnp.exp(jax.random.uniform(keys[2], (H,), minval=math.log(2.0 / TOKENS), maxval=math.log(1.0 / 30.0)))
    head_rate = jnp.where(slow, slow_rate, fast_rate)
    token_multiplier = jnp.exp(jax.random.uniform(keys[3], (TOKENS // TOK_DEV, TOK_DEV, H), minval=-math.log(2.0), maxval=math.log(2.0)))
    block_factor = jnp.exp(jax.random.uniform(keys[4], (TOKENS // TOK_DEV, 1, H), minval=-math.log(2.0), maxval=math.log(2.0)))
    gentle_portion = (head_rate[None, None, :] * token_multiplier * block_factor).reshape(TOKENS, H)
    spots = jax.random.randint(keys[5], (3,), 0, TOKENS)
    objective_entries = jax.random.uniform(keys[6], (3, H), minval=0.22, maxval=0.5)
    agreement_occurrences = (jnp.arange(TOKENS)[:, None] == spots[None, :]).astype(jnp.float32)
    spike_occurrences = jnp.dot(agreement_occurrences, objective_entries)
    return (-gentle_portion - spike_occurrences).astype(jnp.float32)


def with_ends(array, stream_key, low, top_value):
    place = [jax.random.randint(jax.random.fold_in(stream_key, axis), (), 0, length) for axis, length in enumerate(array.shape)]
    main_axis = array.shape.index(max(array.shape))
    neighbour = place[:main_axis] + [(place[main_axis] + 1) % array.shape[main_axis]] + place[main_axis + 1:]
    return array.at[tuple(place)].set(low).at[tuple(neighbour)].set(top_value)


def shard_levels(rng, dims, cuts, smallest, largest):
    gain, own = 1.0, jax.random.fold_in(rng, 6)
    for dim, shards_of in cuts:
        draws = jnp.exp(jax.random.uniform(jax.random.fold_in(own, dim), (shards_of,), jnp.float32, smallest / len(cuts), largest / len(cuts)))
        gain = gain * jnp.repeat(draws, dims[dim] // shards_of).reshape([-1 if axis == dim else 1 for axis in range(len(dims))])
    return gain


def scatter_about(stream_key, shape, scale, reach, pieces=(), held_as=jnp.bfloat16):
    drawn = jax.random.normal(stream_key, shape, jnp.float32) * scale
    if len(pieces) > 0:
        drawn = shard_levels(stream_key, shape, pieces, -0.22, 0.18) * drawn
    return jnp.clip(drawn, min=-reach, max=reach).astype(held_as)


def setup_inputs(seed: int = 0, part: int = 0) -> dict:
    streams_of = jax.random.split(jax.random.key(seed), 14)
    part_keys = jax.random.split(jax.random.fold_in(streams_of[13], part), 14)
    prompt_values = scatter_about(part_keys[0], (TOKENS, H * P_SIZE), 1.0, 6.0, ((0, 4), (1, 4)))
    prompt_keys = scatter_about(part_keys[1], (TOKENS, N), ((N * TOKENS) ** -0.25), 0.31445312, ((0, 4),))
    prompt_queries = scatter_about(part_keys[2], (TOKENS, N), ((N * TOKENS) ** -0.25), 0.31445312, ((0, 4),))
    logarithm_state_decay = draw_logarithm_state_decay(jax.random.fold_in(jax.random.fold_in(streams_of[13], part), 71), part)
    step_values = scatter_about(part_keys[4], (STEPS, BEAMS, H * P_SIZE), 1.0, 6.0, ((1, 4), (2, 4)))
    step_keys = scatter_about(part_keys[5], (STEPS, BEAMS, N), 1.0, 6.0, ((1, 4),))
    step_queries = scatter_about(part_keys[6], (STEPS, BEAMS, N), ((N * TOKENS) ** -0.25), 0.31445312, ((1, 4),))
    step_decay = jnp.clip(-0.6 + 0.58000002 * jax.random.uniform(part_keys[7], (STEPS, BEAMS, H), jnp.float32) ** shard_levels(part_keys[7], (STEPS, BEAMS, H), ((1, 4), (2, 4)), -0.2, 0.2), -0.6, -0.02)
    step_logprob = jnp.clip(-6.0 + 5.95 * jax.random.uniform(part_keys[8], (STEPS, BEAMS), jnp.float32) ** shard_levels(part_keys[8], (STEPS, BEAMS), ((1, 4),), -0.2, 0.2), -6.0, -0.05)
    parents = with_ends(jax.random.randint(part_keys[9], (STEPS, BEAMS), 0, BEAMS), jax.random.fold_in(part_keys[9], 1), 0, BEAMS - 1).astype(jnp.int32)
    finished = with_ends((jax.random.randint(part_keys[10], (STEPS, BEAMS), 0, 3) < 1).astype(jnp.int32), jax.random.fold_in(part_keys[10], 1), 0, 1)
    lengths = with_ends(jax.random.randint(part_keys[11], (BEAMS,), 1, 60), jax.random.fold_in(part_keys[11], 1), 1, 59).astype(jnp.int32)
    init_score = jnp.clip(-20.0 + 18.0 * jax.random.uniform(part_keys[12], (BEAMS,), jnp.float32) ** shard_levels(part_keys[12], (BEAMS,), ((0, 4),), -0.2, 0.2), -20.0, -2.0)
    return {"prompt_values": prompt_values, "prompt_keys": prompt_keys, "prompt_queries": prompt_queries, "logarithm_state_decay": logarithm_state_decay, "step_values": step_values, "step_keys": step_keys, "step_queries": step_queries, "step_decay": step_decay, "step_logprob": step_logprob, "parents": parents, "finished": finished, "lengths": lengths, "init_score": init_score}


def reference(prompt_values, prompt_keys, prompt_queries, logarithm_state_decay, step_values, step_keys, step_queries, step_decay, step_logprob, parents, finished, lengths, init_score):
    block_count = TOKENS // SPAN
    values_blocks = prompt_values.reshape(block_count, SPAN, H, P_SIZE)
    keys_blocks = prompt_keys.reshape(block_count, SPAN, N)
    query_blocks = prompt_queries.reshape(block_count, SPAN, N)
    decay_blocks = logarithm_state_decay.reshape(block_count, SPAN, H)
    lower = jnp.tril(jnp.ones((SPAN, SPAN), dtype=bool))

    def block_step(state_now, item):
        values_one, keys_one, query_one, single_token_decay = item
        sums_one = jnp.cumsum(single_token_decay, axis=0)
        scores = jnp.dot(query_one, keys_one.T, preferred_element_type=jnp.float32)
        spread = jnp.where(lower[:, :, None], sums_one[:, None, :] - sums_one[None, :, :], -jnp.inf)
        weights = (scores[:, :, None] * jnp.exp(spread)).astype(jnp.bfloat16)
        inner = jnp.einsum("ijh,jhp->ihp", weights.astype(jnp.float32), values_one.astype(jnp.float32))
        rounded = state_now.astype(jnp.bfloat16).astype(jnp.float32)
        carried = jnp.einsum("in,hpn->ihp", query_one.astype(jnp.float32), rounded) * jnp.exp(sums_one)[:, :, None]
        output_one = (inner + carried).astype(jnp.bfloat16).reshape(SPAN, H * P_SIZE)
        tail_decay = jnp.exp(sums_one[-1:, :] - sums_one)
        scaled = (values_one.astype(jnp.float32) * tail_decay[:, :, None]).astype(jnp.bfloat16)
        block_state = jnp.einsum("jhp,jn->hpn", scaled.astype(jnp.float32), keys_one.astype(jnp.float32))
        following_memory = jnp.exp(sums_one[-1])[:, None, None] * state_now + block_state
        return following_memory, output_one

    final_state, outputs = lax.scan(block_step, jnp.zeros((H, P_SIZE, N), jnp.float32), (values_blocks, keys_blocks, query_blocks, decay_blocks))
    prompt_output = outputs.reshape(TOKENS, H * P_SIZE)

    state_all = jnp.broadcast_to(final_state[None], (BEAMS, H, P_SIZE, N))
    score_all = init_score
    length_all = lengths.astype(jnp.float32)
    step_list = []
    ranked_list = []
    for step_index in range(STEPS):
        parent_now = parents[step_index]
        state_all = state_all[parent_now]
        score_all = score_all[parent_now]
        length_all = length_all[parent_now]
        done = finished[step_index] == 1
        live = (1 - finished[step_index]).astype(jnp.float32)
        values_now = step_values[step_index].astype(jnp.float32).reshape(BEAMS, H, P_SIZE)
        keys_now = step_keys[step_index].astype(jnp.float32)
        updated = jnp.exp(step_decay[step_index])[:, :, None, None] * state_all + values_now[:, :, :, None] * keys_now[:, None, None, :]
        state_all = jnp.where(done[:, None, None, None], state_all, updated)
        rounded = state_all.astype(jnp.bfloat16).astype(jnp.float32)
        output_now = jnp.einsum("bhpn,bn->bhp", rounded, step_queries[step_index].astype(jnp.float32))
        output_now = jnp.where(done[:, None, None], jnp.float32(0.0), output_now)
        step_list.append(output_now.reshape(BEAMS, H * P_SIZE).astype(jnp.bfloat16))
        score_all = score_all + live * step_logprob[step_index]
        length_all = length_all + live
        normed = score_all / ((5.0 + length_all) / 6.0) ** 0.6
        ranked_list.append(normed - jnp.max(normed))
    step_output = jnp.stack(step_list)
    ranked = jnp.stack(ranked_list)
    beam_states = state_all.reshape(BEAMS, H * P_SIZE, N)
    return prompt_output, step_output, ranked, beam_states
```

```python
import functools

import jax
import jax.numpy as jnp
from jax import lax
from jax.experimental import pallas as pl
from jax.experimental.pallas import tpu as pltpu
from jax.sharding import PartitionSpec as P

LANES = 128
SUB = 8
QUARTERS = 4
F32 = jnp.float32
BF16 = jnp.bfloat16
HIGH = lax.Precision.HIGHEST
TN = (((0,), (0,)), ((), ()))
NT = (((1,), (1,)), ((), ()))

VMEM = pl.BlockSpec(memory_space=pltpu.VMEM)
SMEM = pl.BlockSpec(memory_space=pltpu.SMEM)


def call(body, args, out_shape, in_specs=None, flops=1_000_000, **kwargs):
    return pl.pallas_call(
        body,
        out_shape=out_shape,
        in_specs=in_specs,
        cost_estimate=pl.CostEstimate(flops=flops, bytes_accessed=1_000_000, transcendentals=0),
        **kwargs,
    )(*args)


def iota(shape, axis):
    return lax.broadcasted_iota(jnp.int32, shape, axis)


def head_lanes(heads, first, count, width):
    shape = (heads, count * width)
    return (iota(shape, 0) == first + iota(shape, 1) // width).astype(F32)


def quarter_state(values, keys, sums, first, count, width, out_ref):
    heads = sums.shape[1]
    last = sums[-1:, :]
    tail = jnp.dot(jnp.exp(last - sums), head_lanes(heads, first, count, width), precision=HIGH, preferred_element_type=F32)
    scaled = (values.astype(F32) * tail).astype(BF16)
    rows = count * width
    out_ref[0:rows, :] = lax.dot_general(scaled, keys, TN, preferred_element_type=F32)
    pad = out_ref.shape[0] - rows
    pick = iota((pad, heads), 1) == first + iota((pad, heads), 0)
    total = jnp.sum(jnp.where(pick, last, 0.0), axis=1, keepdims=True)
    out_ref[rows:, :] = jnp.broadcast_to(jnp.exp(total), (pad, LANES))


def first_kernel(quarter_ref, values_ref, keys_ref, decay_ref, sums_ref, out_ref, *, count, width):
    tokens = decay_ref.shape[0]
    lower = (iota((tokens, tokens), 0) >= iota((tokens, tokens), 1)).astype(F32)
    sums = jnp.dot(lower, decay_ref[...], precision=HIGH, preferred_element_type=F32)
    sums_ref[...] = sums
    quarter = quarter_ref[0]
    lanes = count * width
    values = values_ref[:, pl.ds(pl.multiple_of(quarter * lanes, lanes), lanes)]
    quarter_state(values, keys_ref[...], sums, quarter * count, count, width, out_ref)


def rest_kernel(quarter_ref, values_ref, keys_ref, sums_ref, *out_refs, count, width):
    lanes = count * width
    for k, out_ref in enumerate(out_refs):
        quarter = quarter_ref[k + 1]
        values = values_ref[:, pl.ds(pl.multiple_of(quarter * lanes, lanes), lanes)]
        quarter_state(values, keys_ref[...], sums_ref[...], quarter * count, count, width, out_ref)


def inner_kernel(values_ref, keys_ref, queries_ref, sums_ref, out_ref, turned_ref, wide_ref, *, count, width):
    tokens, heads = sums_ref.shape
    half = tokens // 2
    wide_ref[...] = jnp.zeros_like(wide_ref)
    wide_ref[:, 0:heads] = sums_ref[...]
    turned_ref[...] = wide_ref[...].T
    scores = lax.dot_general(queries_ref[...], keys_ref[...], NT, preferred_element_type=F32)
    lower = iota((half, half), 0) >= iota((half, half), 1)
    top = jnp.where(lower, scores[:half, :half], 0.0)
    left = scores[half:, :half]
    bottom = jnp.where(lower, scores[half:, half:], 0.0)
    per_store = LANES // width

    def group(g, carry):
        wide = pltpu.roll(wide_ref[...], lax.rem(LANES - g * count, LANES), 1)
        for k in range(count // per_store):
            place = pl.ds(pl.multiple_of((g * count + k * per_store) * width, LANES), LANES)
            values = values_ref[:, place]
            tops, bottoms = [], []
            for m in range(per_store):
                h = k * per_store + m
                column = wide[:, h : h + 1]
                row = turned_ref[pl.ds(g * count + h, 1), :]
                x = values[:, m * width : (m + 1) * width]
                w0 = (top * jnp.exp(jnp.minimum(column[:half] - row[:, :half], 0.0))).astype(BF16)
                w1 = (left * jnp.exp(column[half:] - row[:, :half])).astype(BF16)
                w2 = (bottom * jnp.exp(jnp.minimum(column[half:] - row[:, half:], 0.0))).astype(BF16)
                tops.append(jnp.dot(w0, x[:half], preferred_element_type=F32))
                bottoms.append(jnp.dot(jnp.concatenate([w1, w2], axis=1), x, preferred_element_type=F32))
            out_ref[0:half, place] = jnp.concatenate(tops, axis=1)
            out_ref[half:, place] = jnp.concatenate(bottoms, axis=1)
        return carry

    lax.fori_loop(0, heads // count, group, 0)


def combine(low, high, out, count, width, decay=True):
    rows = count * width
    for h in range(count):
        place = slice(h * width, (h + 1) * width)
        out[place, :] = high[rows + h : rows + h + 1, :] * low[place, :] + high[place, :]
    if decay:
        out[rows:, :] = low[rows:, :] * high[rows:, :]


def pair_kernel(rank_ref, keep_ref, got_ref, out_ref, *, count, width):
    odd = rank_ref[0] == 1

    @pl.when(odd)
    def _():
        combine(got_ref, keep_ref, out_ref, count, width)

    @pl.when(jnp.logical_not(odd))
    def _():
        combine(keep_ref, got_ref, out_ref, count, width)


def round_kernel(rank_ref, total_ref, got_ref, *refs, bit, first, count, width):
    before_ref, refs = (None, refs) if first else (refs[0], refs[1:])
    before_out, total_out = refs
    upper = rank_ref[bit] == 1
    rows = count * width

    @pl.when(upper)
    def _():
        combine(got_ref, total_ref, total_out, count, width)
        if first:
            before_out[...] = got_ref[...]
        else:
            combine(got_ref, before_ref, before_out, count, width)

    @pl.when(jnp.logical_not(upper))
    def _():
        combine(total_ref, got_ref, total_out, count, width)
        if first:
            before_out[0:rows, :] = jnp.zeros((rows, LANES), F32)
            before_out[rows:, :] = jnp.ones((before_out.shape[0] - rows, LANES), F32)
        else:
            before_out[...] = before_ref[...]


def last_kernel(rank_ref, total_ref, got_ref, keep_ref, swap_ref, *refs, bit, first, pieces, count, width):
    before_ref, refs = (None, refs) if first else (refs[0], refs[1:])
    piece_refs, own_ref, hand_ref, before_now = refs[:pieces], refs[pieces], refs[pieces + 1], refs[pieces + 2]
    upper = rank_ref[bit] == 1
    odd = rank_ref[0] == 1
    rows = count * width
    per_piece = count // pieces

    def final(low, high):
        for h in range(count):
            place = slice(h * width, (h + 1) * width)
            start = (h % per_piece) * width
            piece_refs[h // per_piece][start : start + width, :] = (
                high[rows + h : rows + h + 1, :] * low[place, :] + high[place, :]
            )

    @pl.when(upper)
    def _():
        final(got_ref, total_ref)
        if first:
            before_now[...] = got_ref[0:rows, :]
        else:
            combine(got_ref, before_ref, before_now, count, width, decay=False)

    @pl.when(jnp.logical_not(upper))
    def _():
        final(total_ref, got_ref)
        before_now[...] = jnp.zeros_like(before_now) if first else before_ref[0:rows, :]

    @pl.when(odd)
    def _():
        combine(before_now, swap_ref, own_ref, count, width, decay=False)
        hand_ref[...] = before_now[...]

    @pl.when(jnp.logical_not(odd))
    def _():
        own_ref[...] = before_now[...]
        combine(before_now, keep_ref, hand_ref, count, width, decay=False)


def output_kernel(rank_ref, own_ref, other_ref, queries_ref, sums_ref, inner_ref, *refs, sub, count, width):
    out_ref = refs[-1]
    half = pl.program_id(0)
    heads = sums_ref.shape[1]
    first = (half * 2 + sub) * count

    def emit(state_ref):
        carried = lax.dot_general(queries_ref[...], state_ref[...].astype(BF16), NT, preferred_element_type=F32)
        grown = jnp.dot(
            jnp.exp(sums_ref[...]), head_lanes(heads, first, count, width), precision=HIGH, preferred_element_type=F32
        )
        out_ref[...] = (inner_ref[...] + carried * grown).astype(BF16)

    mine = rank_ref[0] == half

    @pl.when(mine)
    def _():
        emit(own_ref)

    @pl.when(jnp.logical_not(mine))
    def _():
        emit(other_ref)


def lineage_kernel(
    beam_ref, scalar_ref, rows_ref, queries_ref, grow_ref, part_ref, outer_ref, key_ref, shrink_ref, ranked_ref,
    scores, counts, *, slots, steps, wide, width
):
    me = beam_ref[0]
    done = lambda slot, step: scalar_ref[slot * steps + step, 2]
    parent = lambda slot, step: scalar_ref[slot * steps + step, 1].astype(jnp.int32)
    for slot in range(slots):
        scores[0, slot] = scalar_ref[slot * steps, 4]
        counts[0, slot] = scalar_ref[slot * steps, 3]
    lane = iota((1, LANES), 1)
    for step in range(steps):
        score_row = jnp.zeros((1, LANES), F32)
        count_row = jnp.zeros((1, LANES), F32)
        for slot in range(slots):
            source = parent(slot, step)
            live = 1.0 - done(slot, step)
            score = scores[step, source] + live * scalar_ref[slot * steps + step, 0]
            tally = counts[step, source] + live
            scores[step + 1, slot] = score
            counts[step + 1, slot] = tally
            score_row = jnp.where(lane == slot, score, score_row)
            count_row = jnp.where(lane == slot, tally, count_row)
        normed = score_row * jnp.exp(-0.6 * jnp.log((5.0 + count_row) / 6.0))
        best = jnp.max(jnp.where(lane < slots, normed, -jnp.inf), axis=1, keepdims=True)
        mine = jnp.sum(jnp.where(lane == me, normed, 0.0), axis=1, keepdims=True)
        ranked_ref[step : step + 1, :] = jnp.broadcast_to(mine - best, (1, LANES))

    for ref in (grow_ref, part_ref, outer_ref, key_ref):
        ref[...] = jnp.zeros_like(ref)
    for step in range(steps):
        slot = me
        factor = jnp.ones((1, wide), F32)
        part = jnp.zeros((1, wide), F32)
        query = queries_ref[step : step + 1, :].astype(F32)
        live_now = 1.0 - done(me, step)
        for back in range(step, -1, -1):
            record = rows_ref[slot * steps + back]
            live = 1.0 - done(slot, back)
            values = record[:, 0:wide]
            key = record[:, 2 * wide : 2 * wide + LANES]
            weight = factor * (values * live)
            part = part + weight * jnp.sum(key * query, axis=1, keepdims=True)
            if step == steps - 1:
                outer_ref[back : back + 1, :] = weight
                key_ref[back : back + 1, :] = key
            factor = factor * jnp.exp(record[:, wide : 2 * wide] * live)
            slot = parent(slot, back)
        grow_ref[step : step + 1, :] = factor * live_now
        part_ref[step : step + 1, :] = part * live_now
        if step == steps - 1:
            count = shrink_ref.shape[0]
            pick = iota((count, wide), 1) == iota((count, wide), 0) * width
            shrink_ref[...] = jnp.broadcast_to(
                jnp.sum(jnp.where(pick, factor, 0.0), axis=1, keepdims=True), (count, LANES)
            )


def decode_kernel(final_ref, queries_ref, grow_ref, part_ref, outer_ref, key_ref, shrink_ref, *refs, count, width):
    state_ref, out_ref = refs[-2:]
    final = final_ref[...]
    product = lax.dot_general(queries_ref[...], final.astype(BF16), NT, preferred_element_type=F32)
    steps = out_ref.shape[0]
    out_ref[...] = (grow_ref[0:steps, :] * product[0:steps, :] + part_ref[0:steps, :]).astype(BF16)
    fresh = lax.dot_general(outer_ref[...], key_ref[...], TN, precision=HIGH, preferred_element_type=F32)
    for h in range(count):
        place = slice(h * width, (h + 1) * width)
        state_ref[place, :] = shrink_ref[h : h + 1, :] * final[place, :] + fresh[place, :]


def on_device(
    prompt_values, prompt_keys, prompt_queries, logarithm_state_decay, step_values, step_keys, step_queries, step_decay,
    step_logprob, parents, finished, lengths, init_score, *, ranks, slots
):
    tokens, heads = logarithm_state_decay.shape
    width = prompt_values.shape[1] // heads
    steps = step_values.shape[0]
    wide = step_values.shape[2]
    own_heads = wide // width
    count = heads // QUARTERS
    rows = count * width
    message = jax.ShapeDtypeStruct((rows + -(-count // SUB) * SUB, LANES), F32)
    state = jax.ShapeDtypeStruct((rows, LANES), F32)
    sizes = dict(count=count, width=width)
    levels = ranks.bit_length() - 1
    rank = lax.axis_index("seq")
    beam = lax.axis_index("beam").astype(jnp.int32)[None]
    bits = jnp.stack([(rank >> k) & 1 for k in range(levels)]).astype(jnp.int32)
    quarters = jnp.stack([2 - 2 * bits[0], 3 - 2 * bits[0], 2 * bits[0], 2 * bits[0] + 1]).astype(jnp.int32)

    sums, send_a = call(
        functools.partial(first_kernel, **sizes),
        (quarters, prompt_values, prompt_keys, logarithm_state_decay),
        (jax.ShapeDtypeStruct((tokens, heads), F32), message),
        [SMEM, VMEM, VMEM, VMEM],
    )
    swap = [(k, k ^ 1) for k in range(ranks)]
    got_a = lax.ppermute(send_a, "seq", swap)
    send_b, keep_a, keep_b = call(
        functools.partial(rest_kernel, **sizes),
        (quarters, prompt_values, prompt_keys, sums),
        (message,) * 3,
        [SMEM, VMEM, VMEM, VMEM],
    )
    got_b = lax.ppermute(send_b, "seq", swap)
    keeps, swaps = (keep_a, keep_b), (got_a, got_b)

    whole = jnp.concatenate([lengths.astype(F32), init_score])[None]
    scalars = jnp.concatenate(
        [step_logprob, parents.astype(F32), finished.astype(F32), jnp.broadcast_to(whole, (steps, 2))], axis=1
    )
    packed = jnp.concatenate(
        [
            step_values[:, 0].astype(F32),
            jnp.repeat(step_decay[:, 0], width, axis=1),
            step_keys[:, 0].astype(F32),
            jnp.pad(scalars, ((0, 0), (0, LANES - scalars.shape[1]))),
        ],
        axis=1,
    )[:, None, :]
    gathered = lax.all_gather(packed, "beam", axis=0, tiled=True)
    queries = jnp.pad(step_queries[:, 0], ((0, -steps % SUB), (0, 0)))
    line = jax.ShapeDtypeStruct((SUB, wide), F32)
    grow, part, outer, key_rows, shrink, ranked = call(
        functools.partial(lineage_kernel, slots=slots, steps=steps, wide=wide, width=width),
        (beam, gathered[:, 0, 2 * wide + LANES :], gathered, queries),
        (
            line, line, line, jax.ShapeDtypeStruct((SUB, LANES), F32), jax.ShapeDtypeStruct((own_heads, LANES), F32),
            jax.ShapeDtypeStruct((steps, LANES), F32),
        ),
        [SMEM, SMEM, VMEM, VMEM],
        scratch_shapes=[pltpu.SMEM((steps + 1, slots), F32), pltpu.SMEM((steps + 1, slots), F32)],
    )
    ranked = ranked[:, :1]

    inner = call(
        functools.partial(inner_kernel, **sizes),
        (prompt_values, prompt_keys, prompt_queries, sums),
        jax.ShapeDtypeStruct((tokens, heads * width), F32),
        [VMEM] * 4,
        scratch_shapes=[pltpu.VMEM((LANES, tokens), F32), pltpu.VMEM((tokens, LANES), F32)],
        flops=100_000_000,
    )

    direct = ranks == slots
    pieces = slots // 2 if direct else 1
    piece = jax.ShapeDtypeStruct((rows // pieces, LANES), F32)
    out = states = step_out = None
    halves = []
    for sub in range(2):
        total = call(
            functools.partial(pair_kernel, **sizes), (bits, keeps[sub], swaps[sub]), message, [SMEM, VMEM, VMEM]
        )
        before = ()
        for level in range(1, levels):
            got = lax.ppermute(total, "seq", [(k, k ^ (1 << level)) for k in range(ranks)])
            if level < levels - 1:
                before_now, total = call(
                    functools.partial(round_kernel, bit=level, first=level == 1, **sizes),
                    (bits, total, got) + before,
                    (message, message),
                    [SMEM] + [VMEM] * (2 + len(before)),
                )
                before = (before_now,)
        *final, own, hand = call(
            functools.partial(last_kernel, bit=levels - 1, first=levels == 2, pieces=pieces, **sizes),
            (bits, total, got, keeps[sub], swaps[sub]) + before,
            (piece,) * pieces + (state, state),
            [SMEM] + [VMEM] * (4 + len(before)),
            scratch_shapes=[pltpu.VMEM((rows, LANES), F32)],
        )
        halves.append(final)
        if direct:
            landed = None
            for k in range(pieces):
                pairs = [
                    ((g // 2 * 2 + half) * slots + g, g * slots + half * pieces + k)
                    for g in range(ranks)
                    for half in range(2)
                ]
                arrived = lax.ppermute(final[k], ("seq", "beam"), pairs)
                landed = arrived if landed is None else landed + arrived
        back = lax.ppermute(hand, "seq", [(k, k ^ 1) for k in range(1, ranks) if k != 1] + [(0, 1)])
        if direct:
            full = lax.all_gather(landed, "beam", axis=0, tiled=True)
            states, step_out = emit_states(
                full, queries, grow, part, outer, key_rows, shrink, states, step_out, sub, steps, wide, sizes
            )
        columns = pl.BlockSpec((tokens, rows), lambda j, sub=sub: (0, 2 * j + sub))
        out = call(
            functools.partial(output_kernel, sub=sub, **sizes),
            (bits, own, back, prompt_queries, sums, inner) + (() if out is None else (out,)),
            jax.ShapeDtypeStruct((tokens, heads * width), BF16),
            [SMEM] + [VMEM] * 4 + [columns] + ([] if out is None else [pl.BlockSpec(memory_space=pl.ANY)]),
            grid=(2,),
            out_specs=columns,
            input_output_aliases={} if out is None else {6: 0},
        )
    if not direct:
        half = jnp.concatenate([halves[0][0], halves[1][0]])
        other = lax.ppermute(half, "seq", swap)
        first = jnp.where(bits[0] == 0, half, other)
        second = jnp.where(bits[0] == 0, other, half)
        every = lax.all_gather(jnp.concatenate([first, second]), "beam", axis=0, tiled=True)
        full = lax.dynamic_slice_in_dim(every, rank * wide, wide, 0)
        states, step_out = emit_states(
            full, queries, grow, part, outer, key_rows, shrink, None, None, None, steps, wide,
            dict(count=own_heads, width=width)
        )
    return out, step_out.reshape(steps, 1, wide), ranked, states.reshape(1, wide, LANES)


def emit_states(full, queries, grow, part, outer, key_rows, shrink, states, step_out, sub, steps, wide, sizes):
    count, width = sizes["count"], sizes["width"]
    rows = count * width
    at = (lambda j: 0) if sub is None else (lambda j: 2 * j + sub)
    tall = pl.BlockSpec((rows, LANES), lambda j: (at(j), 0))
    flat = lambda height: pl.BlockSpec((height, rows), lambda j: (0, at(j)))
    given = () if states is None else (states, step_out)
    return call(
        functools.partial(decode_kernel, **sizes),
        (full, queries, grow, part, outer, key_rows, shrink) + given,
        (jax.ShapeDtypeStruct((wide, LANES), F32), jax.ShapeDtypeStruct((steps, wide), BF16)),
        [
            pl.BlockSpec((rows, LANES), lambda j: (j, 0)), VMEM, flat(SUB), flat(SUB), flat(SUB), VMEM,
            pl.BlockSpec((count, LANES), lambda j: (at(j), 0)),
        ] + [pl.BlockSpec(memory_space=pl.ANY)] * len(given),
        grid=(1 if sub is None else 2,),
        out_specs=(tall, flat(steps)),
        input_output_aliases={7: 0, 8: 1} if given else {},
    )


def solution(mesh):
    ranks, slots = mesh.shape["seq"], mesh.shape["beam"]
    return jax.shard_map(
        functools.partial(on_device, ranks=ranks, slots=slots),
        mesh=mesh,
        in_specs=(
            P(("groups", "seq"), "beam"),
            P(("groups", "seq"), None),
            P(("groups", "seq"), None),
            P(("groups", "seq"), "beam"),
            P("groups", "beam", "seq"),
            P("groups", "beam", None),
            P("groups", "beam", None),
            P("groups", "beam", "seq"),
            P("groups", "beam"),
            P("groups", "beam"),
            P("groups", "beam"),
            P(("groups", "beam")),
            P(("groups", "beam")),
        ),
        out_specs=(
            P(("groups", "seq"), "beam"),
            P("groups", "beam", "seq"),
            P("groups", "beam"),
            P(("groups", "beam"), "seq", None),
        ),
        check_vma=False,
    )
```

```python
import functools

import jax
import jax.numpy as jnp
from jax import lax
from jax.experimental import pallas as pl
from jax.experimental.pallas import tpu as pltpu
from jax.sharding import PartitionSpec as P


LANES = 128
SUB = 8
QUARTERS = 4
F32 = jnp.float32
BF16 = jnp.bfloat16
HIGH = lax.Precision.HIGHEST
TN = (((0,), (0,)), ((), ()))
NT = (((1,), (1,)), ((), ()))

VMEM = pl.BlockSpec(memory_space=pltpu.VMEM)
HBM = pl.BlockSpec(memory_space=pltpu.HBM)
SMEM = pl.BlockSpec(memory_space=pltpu.SMEM)


def call(body, args, out_shape, in_specs=None, flops=1_000_000, **kwargs):
    return pl.pallas_call(
        body,
        out_shape=out_shape,
        in_specs=in_specs,
        cost_estimate=pl.CostEstimate(flops=flops, bytes_accessed=1_000_000, transcendentals=0),
        compiler_params=pltpu.CompilerParams(vmem_limit_bytes=8 * 2**20),
        **kwargs,
    )(*args)


def gather(array):
    return lax.all_gather(array, "beam", axis=0, tiled=True)


def iota(shape, axis):
    return lax.broadcasted_iota(jnp.int32, shape, axis)


def head_lanes(heads, first, count, width):
    shape = (heads, count * width)
    return (iota(shape, 0) == first + iota(shape, 1) // width).astype(F32)


def quarter_state(values, keys, sums, first, count, width, out_ref):
    heads = sums.shape[1]
    last = sums[-1:, :]
    tail = jnp.dot(jnp.exp(last - sums), head_lanes(heads, first, count, width), precision=HIGH, preferred_element_type=F32)
    scaled = (values.astype(F32) * tail).astype(BF16)
    rows = count * width
    out_ref[0:rows, :] = lax.dot_general(scaled, keys, TN, preferred_element_type=F32)
    pad = out_ref.shape[0] - rows
    pick = iota((pad, heads), 1) == first + iota((pad, heads), 0)
    total = jnp.sum(jnp.where(pick, last, 0.0), axis=1, keepdims=True)
    out_ref[rows:, :] = jnp.broadcast_to(jnp.exp(total), (pad, LANES))


def rank_bit(k):
    return (lax.axis_index("seq") >> k) & 1


def quarter_at(place):
    return ((place // 2) ^ 1 ^ rank_bit(0)) * 2 + place % 2


def fetch(arrived, *pairs):
    copies = [pltpu.make_async_copy(source, target, arrived.at[k]) for k, (source, target) in enumerate(pairs)]
    for copy in copies:
        copy.start()
    return copies


def first_kernel(values_hbm, keys_hbm, decay_hbm, sums_ref, turned_ref, out_ref, values, keys, decay, arrived, *, count, width):
    tokens = decay.shape[1]
    lanes = count * width
    quarter = quarter_at(0)
    columns = values_hbm.at[:, pl.ds(pl.multiple_of(quarter * lanes, lanes), lanes)]
    copies = fetch(arrived, (decay_hbm, decay), (columns, values), (keys_hbm, keys))
    copies[0].wait()
    upper = (iota((tokens, tokens), 0) <= iota((tokens, tokens), 1)).astype(F32)
    turned = jnp.dot(decay[...], upper, precision=HIGH, preferred_element_type=F32)
    turned_ref[...] = turned
    sums = turned.T
    sums_ref[...] = sums
    for copy in copies[1:]:
        copy.wait()
    quarter_state(values[...], keys[...], sums, quarter * count, count, width, out_ref)


def rest_kernel(values_hbm, keys_hbm, sums_ref, *refs, count, width):
    *out_refs, values_ref, keys_ref, arrived = refs
    lanes = count * width
    for copy in fetch(arrived, (values_hbm, values_ref), (keys_hbm, keys_ref)):
        copy.wait()
    for k, out_ref in enumerate(out_refs):
        quarter = quarter_at(k + 1)
        values = values_ref[:, pl.ds(pl.multiple_of(quarter * lanes, lanes), lanes)]
        quarter_state(values, keys_ref[...], sums_ref[...], quarter * count, count, width, out_ref)


def inner_kernel(
    values_hbm, keys_hbm, queries_hbm, sums_ref, turned_ref, out_ref, grown_ref,
    values_ref, keys_ref, queries_ref, wide_ref, arrived, *, count, width
):
    copies = fetch(arrived, (keys_hbm, keys_ref), (queries_hbm, queries_ref), (values_hbm, values_ref))
    tokens, heads = sums_ref.shape
    half = tokens // 2
    wide_ref[...] = jnp.zeros_like(wide_ref)
    wide_ref[:, 0:heads] = sums_ref[...]
    for copy in copies:
        copy.wait()
    scores = lax.dot_general(queries_ref[...], keys_ref[...], NT, preferred_element_type=F32)
    lower = iota((half, half), 0) >= iota((half, half), 1)
    top = jnp.where(lower, scores[:half, :half], 0.0)
    left = scores[half:, :half]
    bottom = jnp.where(lower, scores[half:, half:], 0.0)
    per_store = LANES // width
    lane = iota((tokens, LANES), 1) // width

    def group(g, carry):
        wide = pltpu.roll(wide_ref[...], lax.rem(LANES - g * count, LANES), 1)
        for k in range(count // per_store):
            place = pl.ds(pl.multiple_of((g * count + k * per_store) * width, LANES), LANES)
            values = values_ref[:, place]
            tops, bottoms = [], []
            grown = wide[:, k * per_store : k * per_store + 1]
            for m in range(1, per_store):
                grown = jnp.where(lane == m, wide[:, k * per_store + m : k * per_store + m + 1], grown)
            grown_ref[:, place] = jnp.exp(jnp.broadcast_to(grown, (tokens, LANES)))
            for m in range(per_store):
                h = k * per_store + m
                column = wide[:, h : h + 1]
                row = turned_ref[pl.ds(g * count + h, 1), :]
                x = values[:, m * width : (m + 1) * width]
                w0 = (top * jnp.exp(jnp.minimum(column[:half] - row[:, :half], 0.0))).astype(BF16)
                w1 = (left * jnp.exp(column[half:] - row[:, :half])).astype(BF16)
                w2 = (bottom * jnp.exp(jnp.minimum(column[half:] - row[:, half:], 0.0))).astype(BF16)
                tops.append(jnp.dot(w0, x[:half], preferred_element_type=F32))
                bottoms.append(jnp.dot(jnp.concatenate([w1, w2], axis=1), x, preferred_element_type=F32))
            out_ref[0:half, place] = jnp.concatenate(tops, axis=1)
            out_ref[half:, place] = jnp.concatenate(bottoms, axis=1)
        return carry

    lax.fori_loop(0, heads // count, group, 0)


def combine(low, high, out, count, width, decay=True):
    rows = count * width
    for h in range(count):
        place = slice(h * width, (h + 1) * width)
        out[place, :] = high[rows + h : rows + h + 1, :] * low[place, :] + high[place, :]
    if decay:
        out[rows:, :] = low[rows:, :] * high[rows:, :]


def pair_kernel(keep_ref, got_ref, out_ref, *, count, width):
    odd = rank_bit(0) == 1

    @pl.when(odd)
    def _():
        combine(got_ref, keep_ref, out_ref, count, width)

    @pl.when(jnp.logical_not(odd))
    def _():
        combine(keep_ref, got_ref, out_ref, count, width)


def round_kernel(total_ref, got_ref, *refs, bit, first, count, width):
    before_ref, refs = (None, refs) if first else (refs[0], refs[1:])
    before_out, total_out = refs
    upper = rank_bit(bit) == 1
    rows = count * width

    @pl.when(upper)
    def _():
        combine(got_ref, total_ref, total_out, count, width)
        if first:
            before_out[...] = got_ref[...]
        else:
            combine(got_ref, before_ref, before_out, count, width)

    @pl.when(jnp.logical_not(upper))
    def _():
        combine(total_ref, got_ref, total_out, count, width)
        if first:
            before_out[0:rows, :] = jnp.zeros((rows, LANES), F32)
            before_out[rows:, :] = jnp.ones((before_out.shape[0] - rows, LANES), F32)
        else:
            before_out[...] = before_ref[...]


def last_kernel(total_ref, got_ref, keep_ref, swap_ref, *refs, bit, first, pieces, count, width):
    before_ref, refs = (None, refs) if first else (refs[0], refs[1:])
    piece_refs, own_ref, hand_ref, before_now = refs[:pieces], refs[pieces], refs[pieces + 1], refs[pieces + 2]
    upper = rank_bit(bit) == 1
    odd = rank_bit(0) == 1
    rows = count * width
    per_piece = count // pieces

    def final(low, high):
        for h in range(count):
            place = slice(h * width, (h + 1) * width)
            start = (h % per_piece) * width
            piece_refs[h // per_piece][start : start + width, :] = (
                high[rows + h : rows + h + 1, :] * low[place, :] + high[place, :]
            )

    @pl.when(upper)
    def _():
        final(got_ref, total_ref)
        if first:
            before_now[...] = got_ref[0:rows, :]
        else:
            combine(got_ref, before_ref, before_now, count, width, decay=False)

    @pl.when(jnp.logical_not(upper))
    def _():
        final(total_ref, got_ref)
        before_now[...] = jnp.zeros_like(before_now) if first else before_ref[0:rows, :]

    @pl.when(odd)
    def _():
        combine(before_now, swap_ref, own_ref, count, width, decay=False)
        hand_ref[...] = before_now[...]

    @pl.when(jnp.logical_not(odd))
    def _():
        own_ref[...] = before_now[...]
        combine(before_now, keep_ref, hand_ref, count, width, decay=False)


def output_kernel(own_ref, other_ref, queries_ref, grown_ref, inner_ref, *refs):
    out_ref = refs[-1]

    def emit(state_ref):
        carried = lax.dot_general(queries_ref[...], state_ref[...].astype(BF16), NT, preferred_element_type=F32)
        out_ref[...] = (inner_ref[...] + carried * grown_ref[...]).astype(BF16)

    mine = rank_bit(0) == pl.program_id(0)

    @pl.when(mine)
    def _():
        emit(own_ref)

    @pl.when(jnp.logical_not(mine))
    def _():
        emit(other_ref)


def pack_kernel(values_ref, decay_ref, keys_ref, scalar_ref, tail_ref, out_ref, *, width):
    steps, wide = values_ref.shape
    heads = decay_ref.shape[1]
    out_ref[0, :, 0:wide] = values_ref[...].astype(F32)
    out_ref[0, :, wide : 2 * wide] = jnp.dot(
        decay_ref[...], head_lanes(heads, 0, heads, width), precision=HIGH, preferred_element_type=F32
    )
    out_ref[0, :, 2 * wide : 2 * wide + LANES] = keys_ref[...].astype(F32)
    lane, line = iota((steps, LANES), 1), iota((steps, LANES), 0)
    row = jnp.zeros((steps, LANES), F32)
    for step in range(steps):
        for k in range(scalar_ref.shape[0]):
            row = jnp.where((lane == k) & (line == step), scalar_ref[k, step], row)
    for k in range(tail_ref.shape[0]):
        row = jnp.where(lane == scalar_ref.shape[0] + k, tail_ref[k], row)
    out_ref[0, :, 2 * wide + LANES :] = row


def join_kernel(*refs):
    *parts, out_ref = refs
    out_ref[...] = functools.reduce(lambda a, b: a + b, [part[...] for part in parts])


def lineage_kernel(
    rows_ref, queries_ref, grow_ref, part_ref, fresh_ref, shrink_ref, ranked_ref,
    outer_ref, key_ref, scores, counts, scalar_ref, arrived, *, slots, steps, wide, width
):
    (copy,) = fetch(arrived, (rows_ref.at[:, :, pl.ds(2 * wide + LANES, LANES)], scalar_ref))
    copy.wait()
    me = lax.axis_index("beam")
    ranks_row = jnp.zeros((1, LANES), F32)
    done = lambda slot, step: scalar_ref[slot, step, 2]
    parent = lambda slot, step: scalar_ref[slot, step, 1].astype(jnp.int32)
    for slot in range(slots):
        scores[0, slot] = scalar_ref[slot, 0, 4]
        counts[0, slot] = scalar_ref[slot, 0, 3]
    lane = iota((1, LANES), 1)
    for step in range(steps):
        score_row = jnp.zeros((1, LANES), F32)
        count_row = jnp.zeros((1, LANES), F32)
        for slot in range(slots):
            source = parent(slot, step)
            live = 1.0 - done(slot, step)
            score = scores[step, source] + live * scalar_ref[slot, step, 0]
            tally = counts[step, source] + live
            scores[step + 1, slot] = score
            counts[step + 1, slot] = tally
            score_row = jnp.where(lane == slot, score, score_row)
            count_row = jnp.where(lane == slot, tally, count_row)
        normed = score_row * jnp.exp(-0.6 * jnp.log((5.0 + count_row) / 6.0))
        best = jnp.max(jnp.where(lane < slots, normed, -jnp.inf), axis=1, keepdims=True)
        mine = jnp.sum(jnp.where(lane == me, normed, 0.0), axis=1, keepdims=True)
        ranks_row = jnp.where(lane == step, mine - best, ranks_row)
    ranked_ref[...] = ranks_row[:, 0:steps]

    for ref in (grow_ref, part_ref, outer_ref, key_ref):
        ref[...] = jnp.zeros_like(ref)
    for step in range(steps):
        slot = me
        factor = jnp.ones((1, wide), F32)
        part = jnp.zeros((1, wide), F32)
        query = queries_ref[step : step + 1, :].astype(F32)
        live_now = 1.0 - done(me, step)
        for back in range(step, -1, -1):
            record = rows_ref[slot, back : back + 1, :]
            live = 1.0 - done(slot, back)
            values = record[:, 0:wide]
            key = record[:, 2 * wide : 2 * wide + LANES]
            weight = factor * (values * live)
            part = part + weight * jnp.sum(key * query, axis=1, keepdims=True)
            if step == steps - 1:
                outer_ref[back : back + 1, :] = weight
                key_ref[back : back + 1, :] = key
            factor = factor * jnp.exp(record[:, wide : 2 * wide] * live)
            slot = parent(slot, back)
        grow_ref[step : step + 1, :] = factor * live_now
        part_ref[step : step + 1, :] = part * live_now
        if step == steps - 1:
            fresh_ref[...] = lax.dot_general(outer_ref[...], key_ref[...], TN, precision=HIGH, preferred_element_type=F32)
            count = shrink_ref.shape[0]
            pick = iota((count, wide), 1) == iota((count, wide), 0) * width
            shrink_ref[...] = jnp.broadcast_to(
                jnp.sum(jnp.where(pick, factor, 0.0), axis=1, keepdims=True), (count, LANES)
            )


def decode_kernel(final_ref, queries_ref, grow_ref, part_ref, fresh_ref, shrink_ref, *refs, count, width):
    state_ref, out_ref = refs[-2:]
    final = final_ref[...]
    product = lax.dot_general(queries_ref[...], final.astype(BF16), NT, preferred_element_type=F32)
    steps = out_ref.shape[0]
    out_ref[...] = (grow_ref[0:steps, :] * product[0:steps, :] + part_ref[0:steps, :]).astype(BF16)
    for h in range(count):
        place = slice(h * width, (h + 1) * width)
        state_ref[place, :] = shrink_ref[h : h + 1, :] * final[place, :] + fresh_ref[place, :]


def on_device(
    prompt_values, prompt_keys, prompt_queries, logarithm_state_decay, step_values, step_keys, step_queries, step_decay,
    step_logprob, parents, finished, lengths, init_score, *, ranks, slots
):
    tokens, heads = logarithm_state_decay.shape
    width = prompt_values.shape[1] // heads
    steps = step_values.shape[0]
    wide = step_values.shape[2]
    own_heads = wide // width
    count = heads // QUARTERS
    rows = count * width
    message = jax.ShapeDtypeStruct((rows + -(-count // SUB) * SUB, LANES), F32)
    state = jax.ShapeDtypeStruct((rows, LANES), F32)
    sizes = dict(count=count, width=width)
    levels = ranks.bit_length() - 1
    rank = lax.axis_index("seq")

    turned_shape = jax.ShapeDtypeStruct((heads, tokens), F32)
    sums, turned, send_a = call(
        functools.partial(first_kernel, **sizes),
        (prompt_values, prompt_keys, logarithm_state_decay.T),
        (jax.ShapeDtypeStruct((tokens, heads), F32), turned_shape, message),
        [HBM] * 3,
        scratch_shapes=[
            pltpu.VMEM((tokens, count * width), BF16),
            pltpu.VMEM((tokens, LANES), BF16),
            pltpu.VMEM((heads, tokens), F32),
            pltpu.SemaphoreType.DMA((3,)),
        ],
    )
    swap = [(k, k ^ 1) for k in range(ranks)]
    got_a = lax.ppermute(send_a, "seq", swap)
    send_b, keep_a, keep_b = call(
        functools.partial(rest_kernel, **sizes),
        (prompt_values, prompt_keys, sums),
        (message,) * 3,
        [HBM, HBM, VMEM],
        scratch_shapes=[
            pltpu.VMEM(prompt_values.shape, BF16), pltpu.VMEM((tokens, LANES), BF16), pltpu.SemaphoreType.DMA((2,))
        ],
    )
    got_b = lax.ppermute(send_b, "seq", swap)
    keeps, swaps = (keep_a, keep_b), (got_a, got_b)

    scalars = jnp.concatenate([step_logprob.T, parents.T.astype(F32), finished.T.astype(F32)])
    packed = call(
        functools.partial(pack_kernel, width=width),
        (step_values[:, 0], step_decay[:, 0], step_keys[:, 0], scalars, jnp.concatenate([lengths.astype(F32), init_score])),
        jax.ShapeDtypeStruct((1, steps, 2 * wide + 2 * LANES), F32),
        [VMEM, VMEM, VMEM, SMEM, SMEM],
    )
    gathered = gather(packed)
    queries = step_queries[:, 0]
    line = jax.ShapeDtypeStruct((SUB, wide), F32)
    grow, part, fresh, shrink, ranked = call(
        functools.partial(lineage_kernel, slots=slots, steps=steps, wide=wide, width=width),
        (gathered, queries),
        (
            line, line, jax.ShapeDtypeStruct((wide, LANES), F32), jax.ShapeDtypeStruct((own_heads, LANES), F32),
            jax.ShapeDtypeStruct((1, steps), F32),
        ),
        [VMEM, VMEM],
        scratch_shapes=[
            pltpu.VMEM((SUB, wide), F32), pltpu.VMEM((SUB, LANES), F32),
            pltpu.SMEM((steps + 1, slots), F32), pltpu.SMEM((steps + 1, slots), F32),
            pltpu.SMEM((slots, steps, LANES), F32), pltpu.SemaphoreType.DMA((1,)),
        ],
    )
    ranked = ranked.reshape(steps, 1)

    inner, grown = call(
        functools.partial(inner_kernel, **sizes),
        (prompt_values, prompt_keys, prompt_queries, sums, turned),
        (jax.ShapeDtypeStruct((tokens, heads * width), F32),) * 2,
        [HBM, HBM, HBM, VMEM, VMEM],
        scratch_shapes=[
            pltpu.VMEM(prompt_values.shape, BF16), pltpu.VMEM((tokens, LANES), BF16), pltpu.VMEM((tokens, LANES), BF16),
            pltpu.VMEM((tokens, LANES), F32), pltpu.SemaphoreType.DMA((3,)),
        ],
        flops=100_000_000,
    )

    direct = ranks == slots
    pieces = slots // 2 if direct else 1
    piece = jax.ShapeDtypeStruct((rows // pieces, LANES), F32)
    out = states = step_out = None
    halves = []
    for sub in range(2):
        total = call(functools.partial(pair_kernel, **sizes), (keeps[sub], swaps[sub]), message, [VMEM] * 2)
        before = ()
        for level in range(1, levels):
            got = lax.ppermute(total, "seq", [(k, k ^ (1 << level)) for k in range(ranks)])
            if level < levels - 1:
                before_now, total = call(
                    functools.partial(round_kernel, bit=level, first=level == 1, **sizes),
                    (total, got) + before,
                    (message, message),
                    [VMEM] * (2 + len(before)),
                )
                before = (before_now,)
        *final, own, hand = call(
            functools.partial(last_kernel, bit=levels - 1, first=levels == 2, pieces=pieces, **sizes),
            (total, got, keeps[sub], swaps[sub]) + before,
            (piece,) * pieces + (state, state),
            [VMEM] * (4 + len(before)),
            scratch_shapes=[pltpu.VMEM((rows, LANES), F32)],
        )
        halves.append(final)
        if direct:
            landed = []
            for k in range(pieces):
                pairs = [
                    ((g // 2 * 2 + half) * slots + g, g * slots + half * pieces + k)
                    for g in range(ranks)
                    for half in range(2)
                ]
                landed.append(lax.ppermute(final[k], ("seq", "beam"), pairs))
            landed = call(join_kernel, landed, piece, [VMEM] * pieces)
        back = lax.ppermute(hand, "seq", [(k, k ^ 1) for k in range(1, ranks) if k != 1] + [(0, 1)])
        if direct:
            full = gather(landed)
            states, step_out = emit_states(
                full, queries, grow, part, fresh, shrink, states, step_out, sub, steps, wide, sizes
            )
        columns = pl.BlockSpec((tokens, rows), lambda j, sub=sub: (0, 2 * j + sub))
        out = call(
            output_kernel,
            (own, back, prompt_queries, grown, inner) + (() if out is None else (out,)),
            jax.ShapeDtypeStruct((tokens, heads * width), BF16),
            [VMEM] * 3 + [columns] * 2 + ([] if out is None else [pl.BlockSpec(memory_space=pl.ANY)]),
            grid=(2,),
            out_specs=columns,
            input_output_aliases={} if out is None else {5: 0},
        )
    if not direct:
        half = jnp.concatenate([halves[0][0], halves[1][0]])
        other = lax.ppermute(half, "seq", swap)
        odd = rank_bit(0) == 1
        first, second = jnp.where(odd, other, half), jnp.where(odd, half, other)
        every = lax.all_gather(jnp.concatenate([first, second]), "beam", axis=0, tiled=True)
        full = lax.dynamic_slice_in_dim(every, rank * wide, wide, 0)
        states, step_out = emit_states(
            full, queries, grow, part, fresh, shrink, None, None, None, steps, wide,
            dict(count=own_heads, width=width)
        )
    return out, step_out.reshape(steps, 1, wide), ranked, states.reshape(1, wide, LANES)


def emit_states(full, queries, grow, part, fresh, shrink, states, step_out, sub, steps, wide, sizes):
    count, width = sizes["count"], sizes["width"]
    rows = count * width
    at = (lambda j: 0) if sub is None else (lambda j: 2 * j + sub)
    tall = pl.BlockSpec((rows, LANES), lambda j: (at(j), 0))
    flat = lambda height: pl.BlockSpec((height, rows), lambda j: (0, at(j)))
    given = () if states is None else (states, step_out)
    return call(
        functools.partial(decode_kernel, **sizes),
        (full, queries, grow, part, fresh, shrink) + given,
        (jax.ShapeDtypeStruct((wide, LANES), F32), jax.ShapeDtypeStruct((steps, wide), BF16)),
        [
            pl.BlockSpec((rows, LANES), lambda j: (j, 0)), VMEM, flat(SUB), flat(SUB), tall,
            pl.BlockSpec((count, LANES), lambda j: (at(j), 0)),
        ] + [pl.BlockSpec(memory_space=pl.ANY)] * len(given),
        grid=(1 if sub is None else 2,),
        out_specs=(tall, flat(steps)),
        input_output_aliases={6: 0, 7: 1} if given else {},
    )


def solution(mesh):
    ranks, slots = mesh.shape["seq"], mesh.shape["beam"]

    def body(*args):
        return on_device(*args, ranks=ranks, slots=slots)

    return jax.shard_map(
        body,
        mesh=mesh,
        in_specs=(
            P(("groups", "seq"), "beam"),
            P(("groups", "seq"), None),
            P(("groups", "seq"), None),
            P(("groups", "seq"), "beam"),
            P("groups", "beam", "seq"),
            P("groups", "beam", None),
            P("groups", "beam", None),
            P("groups", "beam", "seq"),
            P("groups", "beam"),
            P("groups", "beam"),
            P("groups", "beam"),
            P(("groups", "beam")),
            P(("groups", "beam")),
        ),
        out_specs=(
            P(("groups", "seq"), "beam"),
            P("groups", "beam", "seq"),
            P("groups", "beam"),
            P(("groups", "beam"), "seq", None),
        ),
        check_vma=False,
    )
```

```python
import functools

import jax
import jax.numpy as jnp
from jax import lax
from jax.experimental import pallas as pl
from jax.experimental.pallas import tpu as pltpu
from jax.sharding import PartitionSpec as P


LANES = 128
SUB = 8
HALVES = 2
SHORT = 2
INNER = 4
F32 = jnp.float32
BF16 = jnp.bfloat16
TN = (((0,), (0,)), ((), ()))
NT = (((1,), (1,)), ((), ()))

VMEM = pl.BlockSpec(memory_space=pltpu.VMEM)
HBM = pl.BlockSpec(memory_space=pltpu.HBM)
SMEM = pl.BlockSpec(memory_space=pltpu.SMEM)


def call(body, args, out_shape, in_specs=None, flops=1_000_000, **kwargs):
    return pl.pallas_call(
        body,
        out_shape=out_shape,
        in_specs=in_specs,
        cost_estimate=pl.CostEstimate(flops=flops, bytes_accessed=1_000_000, transcendentals=0),
        compiler_params=pltpu.CompilerParams(vmem_limit_bytes=8 * 2**20),
        **kwargs,
    )(*args)


def permute(array, axis, pairs):
    return lax.ppermute(array, axis, pairs)


def gather(array):
    return lax.all_gather(array, "beam", axis=0, tiled=True)


def iota(shape, axis):
    return lax.broadcasted_iota(jnp.int32, shape, axis)


def head_lanes(heads, first, count, width):
    shape = (heads, count * width)
    return (iota(shape, 0) == first + iota(shape, 1) // width).astype(F32)


def thirds(x, axis):
    high = x.astype(BF16)
    rest = x - high.astype(F32)
    middle = rest.astype(BF16)
    return jnp.concatenate([high, middle, (rest - middle.astype(F32)).astype(BF16)], axis=axis)


def spread(x, first, count, width):
    hot = head_lanes(x.shape[1], first, count, width).astype(BF16)
    return jnp.dot(thirds(x, 1), jnp.concatenate([hot] * 3, axis=0), preferred_element_type=F32)


def part_state(values, keys, sums, first, count, width, out_ref):
    heads = sums.shape[1]
    last = sums[-1:, :]
    scaled = (values.astype(F32) * spread(jnp.exp(last - sums), first, count, width)).astype(BF16)
    rows = count * width
    out_ref[0:rows, :] = lax.dot_general(scaled, keys, TN, preferred_element_type=F32)
    pad = out_ref.shape[0] - rows
    pick = iota((pad, heads), 1) == first + iota((pad, heads), 0)
    total = jnp.sum(jnp.where(pick, last, 0.0), axis=1, keepdims=True)
    out_ref[rows:, :] = jnp.broadcast_to(jnp.exp(total), (pad, LANES))


def rank_bit(k):
    return (lax.axis_index("seq") >> k) & 1


def half_start(kept, heads):
    return (rank_bit(0) if kept else rank_bit(0) ^ 1) * (heads // HALVES)


def fetch(arrived, *pairs):
    copies = [pltpu.make_async_copy(source, target, arrived.at[k]) for k, (source, target) in enumerate(pairs)]
    for copy in copies:
        copy.start()
    return copies


def first_kernel(values_hbm, keys_hbm, decay_hbm, sums_ref, turned_ref, out_ref, values, keys, decay, arrived, *, count, width):
    heads, tokens = decay.shape
    start = half_start(False, heads)
    columns = values_hbm.at[:, pl.ds(pl.multiple_of(start * width, LANES), count * width)]
    copies = fetch(arrived, (decay_hbm, decay), (columns, values), (keys_hbm, keys))
    copies[0].wait()
    upper = (iota((tokens, tokens), 0) <= iota((tokens, tokens), 1)).astype(F32).astype(BF16)
    terms = jnp.dot(thirds(decay[...], 0), upper, preferred_element_type=F32)
    turned = terms[0:heads] + (terms[heads : 2 * heads] + terms[2 * heads :])
    turned_ref[...] = turned
    sums = turned.T
    sums_ref[...] = sums
    for copy in copies[1:]:
        copy.wait()
    part_state(values[...], keys[...], sums, start, count, width, out_ref)


def state_kernel(values_hbm, keys_hbm, sums_ref, *refs, kept, offset, counts, width):
    *out_refs, values_ref, keys_ref, arrived = refs
    start = half_start(kept, sums_ref.shape[1]) + offset
    columns = pl.ds(pl.multiple_of(start * width, LANES), sum(counts) * width)
    for copy in fetch(arrived, (values_hbm.at[:, columns], values_ref), (keys_hbm, keys_ref)):
        copy.wait()
    done = 0
    for count, out_ref in zip(counts, out_refs, strict=True):
        values = values_ref[:, done * width : (done + count) * width]
        part_state(values, keys_ref[...], sums_ref[...], start + done, count, width, out_ref)
        done += count


def inner_kernel(
    values_hbm, keys_hbm, queries_hbm, sums_ref, turned_ref, out_ref, grown_ref,
    values_ref, keys_ref, queries_ref, wide_ref, arrived, *, count, width
):
    copies = fetch(arrived, (keys_hbm, keys_ref), (queries_hbm, queries_ref), (values_hbm, values_ref))
    tokens, heads = sums_ref.shape
    half = tokens // 2
    wide_ref[...] = jnp.zeros_like(wide_ref)
    wide_ref[:, 0:heads] = sums_ref[...]
    for copy in copies:
        copy.wait()
    scores = lax.dot_general(queries_ref[...], keys_ref[...], NT, preferred_element_type=F32)
    lower = iota((half, half), 0) >= iota((half, half), 1)
    top = jnp.where(lower, scores[:half, :half], 0.0)
    left = scores[half:, :half]
    bottom = jnp.where(lower, scores[half:, half:], 0.0)
    per_store = LANES // width
    lane = iota((tokens, LANES), 1) // width

    def group(g, carry):
        wide = pltpu.roll(wide_ref[...], lax.rem(LANES - g * count, LANES), 1)
        for k in range(count // per_store):
            place = pl.ds(pl.multiple_of((g * count + k * per_store) * width, LANES), LANES)
            values = values_ref[:, place]
            tops, bottoms = [], []
            grown = wide[:, k * per_store : k * per_store + 1]
            for m in range(1, per_store):
                grown = jnp.where(lane == m, wide[:, k * per_store + m : k * per_store + m + 1], grown)
            grown_ref[:, place] = jnp.exp(jnp.broadcast_to(grown, (tokens, LANES)))
            for m in range(per_store):
                h = k * per_store + m
                column = wide[:, h : h + 1]
                row = turned_ref[pl.ds(g * count + h, 1), :]
                x = values[:, m * width : (m + 1) * width]
                w0 = (top * jnp.exp(jnp.minimum(column[:half] - row[:, :half], 0.0))).astype(BF16)
                w1 = (left * jnp.exp(column[half:] - row[:, :half])).astype(BF16)
                w2 = (bottom * jnp.exp(jnp.minimum(column[half:] - row[:, half:], 0.0))).astype(BF16)
                tops.append(jnp.dot(w0, x[:half], preferred_element_type=F32))
                bottoms.append(jnp.dot(jnp.concatenate([w1, w2], axis=1), x, preferred_element_type=F32))
            out_ref[0:half, place] = jnp.concatenate(tops, axis=1)
            out_ref[half:, place] = jnp.concatenate(bottoms, axis=1)
        return carry

    lax.fori_loop(0, heads // count, group, 0)


def combine(low, high, out, count, width, decay=True):
    rows = count * width
    for h in range(count):
        place = slice(h * width, (h + 1) * width)
        out[place, :] = high[rows + h : rows + h + 1, :] * low[place, :] + high[place, :]
    if decay:
        out[rows:, :] = low[rows:, :] * high[rows:, :]


def pair_kernel(keep_ref, got_ref, out_ref, *, count, width):
    odd = rank_bit(0) == 1

    @pl.when(odd)
    def _():
        combine(got_ref, keep_ref, out_ref, count, width)

    @pl.when(jnp.logical_not(odd))
    def _():
        combine(keep_ref, got_ref, out_ref, count, width)


def round_kernel(total_ref, got_ref, *refs, bit, first, count, width):
    before_ref, refs = (None, refs) if first else (refs[0], refs[1:])
    before_out, total_out = refs
    upper = rank_bit(bit) == 1
    rows = count * width

    @pl.when(upper)
    def _():
        combine(got_ref, total_ref, total_out, count, width)
        if first:
            before_out[...] = got_ref[...]
        else:
            combine(got_ref, before_ref, before_out, count, width)

    @pl.when(jnp.logical_not(upper))
    def _():
        combine(total_ref, got_ref, total_out, count, width)
        if first:
            before_out[0:rows, :] = jnp.zeros((rows, LANES), F32)
            before_out[rows:, :] = jnp.ones((before_out.shape[0] - rows, LANES), F32)
        else:
            before_out[...] = before_ref[...]


def last_kernel(total_ref, got_ref, keep_ref, swap_ref, *refs, bit, first, count, width):
    before_ref, refs = (None, refs) if first else (refs[0], refs[1:])
    final_ref, own_ref, hand_ref, before_now = refs
    upper = rank_bit(bit) == 1
    odd = rank_bit(0) == 1
    rows = count * width

    @pl.when(upper)
    def _():
        combine(got_ref, total_ref, final_ref, count, width, decay=False)
        if first:
            before_now[...] = got_ref[0:rows, :]
        else:
            combine(got_ref, before_ref, before_now, count, width, decay=False)

    @pl.when(jnp.logical_not(upper))
    def _():
        combine(total_ref, got_ref, final_ref, count, width, decay=False)
        before_now[...] = jnp.zeros_like(before_now) if first else before_ref[0:rows, :]

    @pl.when(odd)
    def _():
        combine(before_now, swap_ref, own_ref, count, width, decay=False)
        hand_ref[...] = before_now[...]

    @pl.when(jnp.logical_not(odd))
    def _():
        own_ref[...] = before_now[...]
        combine(before_now, keep_ref, hand_ref, count, width, decay=False)


def output_kernel(own_ref, other_ref, queries_ref, grown_ref, inner_ref, *refs, offset, width):
    out_hbm, held, sent = refs[-3:]
    lanes = own_ref.shape[0]
    copies = []
    for half in range(HALVES):
        columns = slice(half * out_hbm.shape[1] // HALVES + offset * width, None)
        columns = slice(columns.start, columns.start + lanes)

        def emit(state_ref):
            carried = lax.dot_general(queries_ref[...], state_ref[...].astype(BF16), NT, preferred_element_type=F32)
            held[half] = (inner_ref[:, columns] + carried * grown_ref[:, columns]).astype(BF16)

        mine = rank_bit(0) == half

        @pl.when(mine)
        def _():
            emit(own_ref)

        @pl.when(jnp.logical_not(mine))
        def _():
            emit(other_ref)

        copies.append(pltpu.make_async_copy(held.at[half], out_hbm.at[:, pl.ds(columns.start, lanes)], sent.at[half]))
        copies[-1].start()
    for copy in copies:
        copy.wait()


def pack_kernel(
    values_ref, decay_ref, keys_ref, score_ref, parent_ref, done_ref, length_ref, first_ref, out_ref, *, width
):
    steps, wide = values_ref.shape
    heads = decay_ref.shape[1]
    decays = spread(decay_ref[...], 0, heads, width)
    values = values_ref[...].astype(F32)
    lane = iota((1, LANES), 1)
    lines = wide // LANES
    for step in range(steps):
        row = jnp.zeros((1, LANES), F32)
        for k, ref in enumerate((score_ref, parent_ref, done_ref, length_ref, first_ref)):
            place = step if ref.shape[1] > 1 else 0
            row = jnp.where(lane == k, ref[0:1, place : place + 1].astype(F32), row)
        out_ref[step : step + 1, :] = row
        start = 2 * steps + step * 2 * lines
        for k in range(lines):
            lanes = slice(k * LANES, (k + 1) * LANES)
            out_ref[start + k : start + k + 1, :] = values[step : step + 1, lanes]
            out_ref[start + lines + k : start + lines + k + 1, :] = decays[step : step + 1, lanes]
    out_ref[steps : 2 * steps, :] = keys_ref[...].astype(F32)


def whole_kernel(final_ref, next_ref, far_ref, out_ref):
    home = lax.axis_index("seq") == lax.axis_index("beam")
    for half in range(HALVES):
        local = rank_bit(0) == half

        @pl.when(home & local)
        def _():
            out_ref[half] = final_ref[...]

        @pl.when(home ^ local)
        def _():
            out_ref[half] = next_ref[...]

        @pl.when(jnp.logical_not(home | local))
        def _():
            out_ref[half] = far_ref[...]


def either_kernel(mine_ref, got_ref, out_ref, *, bits):
    has = ((lax.axis_index("seq") ^ lax.axis_index("beam")) & bits) == 0

    @pl.when(has)
    def _():
        out_ref[...] = mine_ref[...]

    @pl.when(jnp.logical_not(has))
    def _():
        out_ref[...] = got_ref[...]


def lineage_kernel(
    rows_ref, queries_ref, grow_ref, part_ref, fresh_ref, shrink_ref, ranked_ref,
    outer_ref, key_ref, scores, counts, scalar_ref, arrived, *, slots, steps, wide, width
):
    (copy,) = fetch(arrived, (rows_ref.at[:, pl.ds(0, 2 * steps), :], scalar_ref))
    copy.wait()
    lines = wide // LANES
    flat = lambda x: jnp.concatenate([x[k : k + 1, :] for k in range(lines)], axis=1)
    me = lax.axis_index("beam")
    ranks_row = jnp.zeros((1, LANES), F32)
    done = lambda slot, step: scalar_ref[slot, step, 2]
    parent = lambda slot, step: scalar_ref[slot, step, 1].astype(jnp.int32)
    for slot in range(slots):
        scores[0, slot] = scalar_ref[slot, 0, 4]
        counts[0, slot] = scalar_ref[slot, 0, 3]
    lane = iota((1, LANES), 1)
    for step in range(steps):
        score_row = jnp.zeros((1, LANES), F32)
        count_row = jnp.zeros((1, LANES), F32)
        for slot in range(slots):
            source = parent(slot, step)
            live = 1.0 - done(slot, step)
            score = scores[step, source] + live * scalar_ref[slot, step, 0]
            tally = counts[step, source] + live
            scores[step + 1, slot] = score
            counts[step + 1, slot] = tally
            score_row = jnp.where(lane == slot, score, score_row)
            count_row = jnp.where(lane == slot, tally, count_row)
        normed = score_row * jnp.exp(-0.6 * jnp.log((5.0 + count_row) / 6.0))
        best = jnp.max(jnp.where(lane < slots, normed, -jnp.inf), axis=1, keepdims=True)
        mine = jnp.sum(jnp.where(lane == me, normed, 0.0), axis=1, keepdims=True)
        ranks_row = jnp.where(lane == step, mine - best, ranks_row)
    ranked_ref[...] = ranks_row[:, 0:steps]

    for ref in (grow_ref, part_ref, outer_ref, key_ref):
        ref[...] = jnp.zeros_like(ref)
    for step in range(steps):
        slot = me
        factor = jnp.ones((lines, LANES), F32)
        part = jnp.zeros((lines, LANES), F32)
        query = queries_ref[step : step + 1, :].astype(F32)
        live_now = 1.0 - done(me, step)
        for back in range(step, -1, -1):
            start = 2 * steps + back * 2 * lines
            live = 1.0 - done(slot, back)
            values = rows_ref[slot, start : start + lines, :]
            key = rows_ref[slot, steps + back : steps + back + 1, :]
            weight = factor * (values * live)
            part = part + weight * jnp.sum(key * query, axis=1, keepdims=True)
            if step == steps - 1:
                outer_ref[back : back + 1, :] = flat(weight)
                key_ref[back : back + 1, :] = key
            factor = factor * jnp.exp(rows_ref[slot, start + lines : start + 2 * lines, :] * live)
            slot = parent(slot, back)
        grow_ref[step : step + 1, :] = flat(factor * live_now)
        part_ref[step : step + 1, :] = flat(part * live_now)
        if step == steps - 1:
            keys = jnp.concatenate([key_ref[...].astype(BF16)] * 3, axis=0)
            fresh_ref[...] = lax.dot_general(thirds(outer_ref[...], 0), keys, TN, preferred_element_type=F32)
            count = shrink_ref.shape[0]
            pick = iota((count, wide), 1) == iota((count, wide), 0) * width
            shrink_ref[...] = jnp.broadcast_to(
                jnp.sum(jnp.where(pick, flat(factor), 0.0), axis=1, keepdims=True), (count, LANES)
            )


def decode_kernel(
    final_ref, queries_ref, grow_ref, part_ref, fresh_ref, shrink_ref, *refs, stretches, offset, count, width, last, given
):
    if given:
        earlier_ref, refs = refs[0], refs[2:]
    states_hbm, out_ref, held, sent = refs
    steps = queries_ref.shape[0]
    rows = count * width
    stretch = grow_ref.shape[1] // stretches
    copies = []
    for k in range(stretches):
        start = k * stretch + offset * width
        final = final_ref[k]
        product = lax.dot_general(queries_ref[...], final.astype(BF16), NT, preferred_element_type=F32)
        lanes = slice(start, start + rows)
        result = (grow_ref[0:steps, lanes] * product + part_ref[0:steps, lanes]).astype(BF16)
        if last:
            out_ref[:, lanes] = result
        else:
            out_ref[:, k * rows : (k + 1) * rows] = result
        for h in range(count):
            inside = slice(h * width, (h + 1) * width)
            head = start // width + h
            held[k, inside, :] = (
                shrink_ref[head : head + 1, :] * final[inside, :] + fresh_ref[start + h * width : start + (h + 1) * width, :]
            )
        copies.append(pltpu.make_async_copy(held.at[k], states_hbm.at[pl.ds(start, rows), :], sent.at[k]))
        copies[-1].start()
        if given:
            before = earlier_ref.shape[1] // stretches
            out_ref[:, k * stretch : k * stretch + before] = earlier_ref[:, k * before : (k + 1) * before]
    for copy in copies:
        copy.wait()


def emit_states(final, offset, count, width, lines, earlier, last):
    wide, steps = lines[1].shape[1], lines[0].shape[0]
    rows, stretches = count * width, final.shape[0]
    given = () if earlier is None else (earlier[1], earlier[0])
    return call(
        functools.partial(
            decode_kernel, stretches=stretches, offset=offset, count=count, width=width, last=last, given=bool(given)
        ),
        (final,) + lines + given,
        (
            jax.ShapeDtypeStruct((wide, LANES), F32),
            jax.ShapeDtypeStruct((steps, wide if last else stretches * rows), BF16),
        ),
        [VMEM] * 6 + [VMEM, HBM][: len(given)],
        out_specs=(HBM, VMEM),
        scratch_shapes=[pltpu.VMEM((stretches, rows, LANES), F32), pltpu.SemaphoreType.DMA((stretches,))],
        input_output_aliases={7: 0} if given else {},
    )


def on_device(
    prompt_values, prompt_keys, prompt_queries, logarithm_state_decay, step_values, step_keys, step_queries, step_decay,
    step_logprob, parents, finished, lengths, init_score, *, ranks, slots
):
    here = lambda x: pltpu.with_memory_space_constraint(x, pltpu.HBM)
    prompt_values, prompt_keys, prompt_queries = here(prompt_values), here(prompt_keys), here(prompt_queries)
    tokens, heads = logarithm_state_decay.shape
    width = prompt_values.shape[1] // heads
    steps = step_values.shape[0]
    wide = step_values.shape[2]
    own_heads = wide // width
    half_heads = heads // HALVES
    counts = (half_heads // SHORT, half_heads - half_heads // SHORT)
    offsets = (0, counts[0])
    array = lambda *shape, dtype=F32: jax.ShapeDtypeStruct(shape, dtype)
    messages = [array(count * width + -(-count // SUB) * SUB, LANES) for count in counts]
    levels = ranks.bit_length() - 1
    rank = lax.axis_index("seq")

    sums, turned, send_a = call(
        functools.partial(first_kernel, count=counts[0], width=width),
        (prompt_values, prompt_keys, here(logarithm_state_decay.T)),
        (array(tokens, heads), array(heads, tokens), messages[0]),
        [HBM] * 3,
        scratch_shapes=[
            pltpu.VMEM((tokens, counts[0] * width), BF16), pltpu.VMEM((tokens, LANES), BF16), pltpu.VMEM((heads, tokens), F32),
            pltpu.SemaphoreType.DMA((3,)),
        ],
    )
    swap = [(k, k ^ 1) for k in range(ranks)]
    got_a = permute(send_a, "seq", swap)

    def more_states(kept, offset, parts):
        return call(
            functools.partial(state_kernel, kept=kept, offset=offset, counts=[counts[sub] for sub in parts], width=width),
            (prompt_values, prompt_keys, sums),
            [messages[sub] for sub in parts],
            [HBM, HBM, VMEM],
            scratch_shapes=[
                pltpu.VMEM((tokens, sum(counts[sub] for sub in parts) * width), BF16), pltpu.VMEM((tokens, LANES), BF16),
                pltpu.SemaphoreType.DMA((2,)),
            ],
        )

    (send_b,) = more_states(False, offsets[1], (1,))
    got_b = permute(send_b, "seq", swap)
    keep_a, keep_b = more_states(True, 0, (0, 1))
    keeps, swaps = (keep_a, keep_b), (got_a, got_b)

    packed = call(
        functools.partial(pack_kernel, width=width),
        (
            step_values[:, 0], step_decay[:, 0], step_keys[:, 0], step_logprob.T, parents.T, finished.T, lengths[None],
            init_score[None],
        ),
        array(2 * steps * (1 + wide // LANES), LANES),
        [VMEM] * 8,
    )
    queries = step_queries[:, 0]

    *lines, ranked = call(
        functools.partial(lineage_kernel, slots=slots, steps=steps, wide=wide, width=width),
        (gather(packed).reshape(slots, -1, LANES), queries),
        (array(SUB, wide), array(SUB, wide), array(wide, LANES), array(own_heads, LANES), array(1, steps)),
        [VMEM, VMEM],
        scratch_shapes=[
            pltpu.VMEM((SUB, wide), F32), pltpu.VMEM((SUB, LANES), F32),
            pltpu.SMEM((steps + 1, slots), F32), pltpu.SMEM((steps + 1, slots), F32),
            pltpu.SMEM((slots, 2 * steps, LANES), F32), pltpu.SemaphoreType.DMA((1,)),
        ],
    )
    lines, ranked = (queries, *lines), ranked.reshape(steps, 1)

    inner, grown = call(
        functools.partial(inner_kernel, count=heads // INNER, width=width),
        (prompt_values, prompt_keys, prompt_queries, sums, turned),
        (array(tokens, heads * width),) * 2,
        [HBM, HBM, HBM, VMEM, VMEM],
        scratch_shapes=[
            pltpu.VMEM(prompt_values.shape, BF16), pltpu.VMEM((tokens, LANES), BF16), pltpu.VMEM((tokens, LANES), BF16),
            pltpu.VMEM((tokens, LANES), F32), pltpu.SemaphoreType.DMA((3,)),
        ],
        flops=100_000_000,
    )

    direct = ranks == slots
    out = states = step_out = None
    finals = []
    for sub, count in enumerate(counts):
        sizes = dict(count=count, width=width)
        rows, message = count * width, messages[sub]
        total = call(functools.partial(pair_kernel, **sizes), (keeps[sub], swaps[sub]), message, [VMEM] * 2)
        before = ()
        for level in range(1, levels):
            got = permute(total, "seq", [(k, k ^ (1 << level)) for k in range(ranks)])
            if level < levels - 1:
                before_now, total = call(
                    functools.partial(round_kernel, bit=level, first=level == 1, **sizes),
                    (total, got) + before,
                    (message, message),
                    [VMEM] * (2 + len(before)),
                )
                before = (before_now,)
        final, own, hand = call(
            functools.partial(last_kernel, bit=levels - 1, first=levels == 2, **sizes),
            (total, got, keeps[sub], swaps[sub]) + before,
            (array(rows, LANES),) * 3,
            [VMEM] * (4 + len(before)),
            scratch_shapes=[pltpu.VMEM((rows, LANES), F32)],
        )
        finals.append(final)
        if direct:
            far = slots // HALVES
            near = [((g ^ 1) * slots + g, g * slots + g) for g in range(ranks)]
            near += [(g * slots + g, g * slots + (g ^ far)) for g in range(ranks)]
            across = permute(final, ("seq", "beam"), [((g ^ 1) * slots + g, g * slots + (g ^ far)) for g in range(ranks)])
            came = permute(final, ("seq", "beam"), near)
            full = call(whole_kernel, (final, came, across), array(HALVES, rows, LANES), [VMEM] * 3)
            bit = 1
            while bit < far:
                have = [b for b in range(slots) if b & (far - 1) < bit]
                pairs = [(g * slots + (g ^ b), g * slots + (g ^ b ^ bit)) for g in range(ranks) for b in have]
                handed = permute(full, ("seq", "beam"), pairs)
                full = call(
                    functools.partial(either_kernel, bits=bit), (full, handed), array(HALVES, rows, LANES),
                    [VMEM] * 2,
                )
                bit *= 2
        back = permute(hand, "seq", [(k, k ^ 1) for k in range(1, ranks) if k != 1] + [(0, 1)])
        if direct:
            states, step_out = emit_states(
                full, offsets[sub], count, width, lines, (states, step_out) if sub else None, sub == 1
            )
        given = () if out is None else (out,)
        out = call(
            functools.partial(output_kernel, offset=offsets[sub], width=width),
            (own, back, prompt_queries, grown, inner) + given,
            array(tokens, heads * width, dtype=BF16),
            [VMEM] * 5 + [HBM] * len(given),
            out_specs=HBM,
            scratch_shapes=[pltpu.VMEM((HALVES, tokens, rows), BF16), pltpu.SemaphoreType.DMA((HALVES,))],
            input_output_aliases={5: 0} if given else {},
        )
    if not direct:
        half = jnp.concatenate(finals)
        other = lax.ppermute(half, "seq", swap)
        odd = rank_bit(0) == 1
        both = jnp.concatenate([jnp.where(odd, other, half), jnp.where(odd, half, other)])
        every = gather(both)
        full = lax.dynamic_slice_in_dim(every, rank * wide, wide, 0)[None]
        states, step_out = emit_states(full, 0, own_heads, width, lines, None, True)
    return out, step_out.reshape(steps, 1, wide), ranked, states.reshape(1, wide, LANES)


def solution(mesh):
    ranks, slots = mesh.shape["seq"], mesh.shape["beam"]

    def body(*args):
        return on_device(*args, ranks=ranks, slots=slots)

    return jax.shard_map(
        body,
        mesh=mesh,
        in_specs=(
            P(("groups", "seq"), "beam"),
            P(("groups", "seq"), None),
            P(("groups", "seq"), None),
            P(("groups", "seq"), "beam"),
            P("groups", "beam", "seq"),
            P("groups", "beam", None),
            P("groups", "beam", None),
            P("groups", "beam", "seq"),
            P("groups", "beam"),
            P("groups", "beam"),
            P("groups", "beam"),
            P(("groups", "beam")),
            P(("groups", "beam")),
        ),
        out_specs=(
            P(("groups", "seq"), "beam"),
            P("groups", "beam", "seq"),
            P("groups", "beam"),
            P(("groups", "beam"), "seq", None),
        ),
        check_vma=False,
    )
```

```python
import functools

import jax
import jax.numpy as jnp
from jax import lax
from jax.experimental import pallas as pl
from jax.experimental.pallas import tpu as pltpu
from jax.sharding import PartitionSpec as P


LANES = 128
SUB = 8
HALVES = 2
SHARE = 3 / 8
INNER = 4
F32 = jnp.float32
BF16 = jnp.bfloat16
TN = (((0,), (0,)), ((), ()))
NT = (((1,), (1,)), ((), ()))

VMEM = pl.BlockSpec(memory_space=pltpu.VMEM)
HBM = pl.BlockSpec(memory_space=pltpu.HBM)
SMEM = pl.BlockSpec(memory_space=pltpu.SMEM)


def call(body, args, out_shape, in_specs=None, flops=1_000_000, **kwargs):
    return pl.pallas_call(
        body,
        out_shape=out_shape,
        in_specs=in_specs,
        cost_estimate=pl.CostEstimate(flops=flops, bytes_accessed=1_000_000, transcendentals=0),
        compiler_params=pltpu.CompilerParams(vmem_limit_bytes=8 * 2**20),
        **kwargs,
    )(*args)


def permute(array, axis, pairs):
    return lax.ppermute(array, axis, pairs)


def gather(array):
    return lax.all_gather(array, "beam", axis=0, tiled=True)


def iota(shape, axis):
    return lax.broadcasted_iota(jnp.int32, shape, axis)


def head_lanes(heads, first, count, width):
    shape = (heads, count * width)
    return (iota(shape, 0) == first + iota(shape, 1) // width).astype(F32)


def thirds(x, axis):
    high = x.astype(BF16)
    rest = x - high.astype(F32)
    middle = rest.astype(BF16)
    return jnp.concatenate([high, middle, (rest - middle.astype(F32)).astype(BF16)], axis=axis)


def spread(x, first, count, width):
    hot = head_lanes(x.shape[1], first, count, width).astype(BF16)
    return jnp.dot(thirds(x, 1), jnp.concatenate([hot] * 3, axis=0), preferred_element_type=F32)


def part_state(values, keys, sums, first, count, width, out_ref):
    heads = sums.shape[1]
    last = sums[-1:, :]
    scaled = (values.astype(F32) * spread(jnp.exp(last - sums), first, count, width)).astype(BF16)
    rows = count * width
    out_ref[0:rows, :] = lax.dot_general(scaled, keys, TN, preferred_element_type=F32)
    pad = out_ref.shape[0] - rows
    pick = iota((pad, heads), 1) == first + iota((pad, heads), 0)
    total = jnp.sum(jnp.where(pick, last, 0.0), axis=1, keepdims=True)
    out_ref[rows:, :] = jnp.broadcast_to(jnp.exp(total), (pad, LANES))


def rank_bit(k):
    return (lax.axis_index("seq") >> k) & 1


def half_start(kept, heads):
    return (rank_bit(0) if kept else rank_bit(0) ^ 1) * (heads // HALVES)


def fetch(arrived, *pairs):
    copies = [pltpu.make_async_copy(source, target, arrived.at[k]) for k, (source, target) in enumerate(pairs)]
    for copy in copies:
        copy.start()
    return copies


def first_kernel(values_hbm, keys_hbm, decay_hbm, sums_ref, turned_ref, out_ref, values, keys, decay, arrived, *, count, width):
    heads, tokens = decay.shape
    start = half_start(False, heads)
    columns = values_hbm.at[:, pl.ds(pl.multiple_of(start * width, LANES), count * width)]
    copies = fetch(arrived, (decay_hbm, decay), (columns, values), (keys_hbm, keys))
    copies[0].wait()
    upper = (iota((tokens, tokens), 0) <= iota((tokens, tokens), 1)).astype(F32).astype(BF16)
    terms = jnp.dot(thirds(decay[...], 0), upper, preferred_element_type=F32)
    turned = terms[0:heads] + (terms[heads : 2 * heads] + terms[2 * heads :])
    turned_ref[...] = turned
    sums = turned.T
    sums_ref[...] = sums
    for copy in copies[1:]:
        copy.wait()
    part_state(values[...], keys[...], sums, start, count, width, out_ref)


def state_kernel(values_hbm, keys_hbm, sums_ref, *refs, kept, offset, counts, width):
    *out_refs, values_ref, keys_ref, arrived = refs
    start = half_start(kept, sums_ref.shape[1]) + offset
    columns = pl.ds(pl.multiple_of(start * width, LANES), sum(counts) * width)
    for copy in fetch(arrived, (values_hbm.at[:, columns], values_ref), (keys_hbm, keys_ref)):
        copy.wait()
    done = 0
    for count, out_ref in zip(counts, out_refs, strict=True):
        values = values_ref[:, done * width : (done + count) * width]
        part_state(values, keys_ref[...], sums_ref[...], start + done, count, width, out_ref)
        done += count


def inner_kernel(
    values_hbm, keys_hbm, queries_hbm, sums_ref, turned_ref, out_ref, grown_ref,
    values_ref, keys_ref, queries_ref, wide_ref, arrived, *, count, width
):
    copies = fetch(arrived, (keys_hbm, keys_ref), (queries_hbm, queries_ref), (values_hbm, values_ref))
    tokens, heads = sums_ref.shape
    half = tokens // 2
    wide_ref[...] = jnp.zeros_like(wide_ref)
    wide_ref[:, 0:heads] = sums_ref[...]
    for copy in copies:
        copy.wait()
    scores = lax.dot_general(queries_ref[...], keys_ref[...], NT, preferred_element_type=F32)
    lower = iota((half, half), 0) >= iota((half, half), 1)
    top = jnp.where(lower, scores[:half, :half], 0.0)
    left = scores[half:, :half]
    bottom = jnp.where(lower, scores[half:, half:], 0.0)
    per_store = LANES // width
    lane = iota((tokens, LANES), 1) // width

    def group(g, carry):
        wide = pltpu.roll(wide_ref[...], lax.rem(LANES - g * count, LANES), 1)
        for k in range(count // per_store):
            place = pl.ds(pl.multiple_of((g * count + k * per_store) * width, LANES), LANES)
            values = values_ref[:, place]
            tops, bottoms = [], []
            grown = wide[:, k * per_store : k * per_store + 1]
            for m in range(1, per_store):
                grown = jnp.where(lane == m, wide[:, k * per_store + m : k * per_store + m + 1], grown)
            grown_ref[:, place] = jnp.exp(jnp.broadcast_to(grown, (tokens, LANES)))
            for m in range(per_store):
                h = k * per_store + m
                column = wide[:, h : h + 1]
                row = turned_ref[pl.ds(g * count + h, 1), :]
                x = values[:, m * width : (m + 1) * width]
                w0 = (top * jnp.exp(jnp.minimum(column[:half] - row[:, :half], 0.0))).astype(BF16)
                w1 = (left * jnp.exp(column[half:] - row[:, :half])).astype(BF16)
                w2 = (bottom * jnp.exp(jnp.minimum(column[half:] - row[:, half:], 0.0))).astype(BF16)
                tops.append(jnp.dot(w0, x[:half], preferred_element_type=F32))
                bottoms.append(jnp.dot(jnp.concatenate([w1, w2], axis=1), x, preferred_element_type=F32))
            out_ref[0:half, place] = jnp.concatenate(tops, axis=1)
            out_ref[half:, place] = jnp.concatenate(bottoms, axis=1)
        return carry

    lax.fori_loop(0, heads // count, group, 0)


def combine(low, high, out, count, width, decay=True):
    rows = count * width
    for h in range(count):
        place = slice(h * width, (h + 1) * width)
        out[place, :] = high[rows + h : rows + h + 1, :] * low[place, :] + high[place, :]
    if decay:
        out[rows:, :] = low[rows:, :] * high[rows:, :]


def pair_kernel(keep_ref, got_ref, out_ref, *, count, width):
    odd = rank_bit(0) == 1

    @pl.when(odd)
    def _():
        combine(got_ref, keep_ref, out_ref, count, width)

    @pl.when(jnp.logical_not(odd))
    def _():
        combine(keep_ref, got_ref, out_ref, count, width)


def round_kernel(total_ref, got_ref, *refs, bit, first, count, width):
    before_ref, refs = (None, refs) if first else (refs[0], refs[1:])
    before_out, total_out = refs
    upper = rank_bit(bit) == 1
    rows = count * width

    @pl.when(upper)
    def _():
        combine(got_ref, total_ref, total_out, count, width)
        if first:
            before_out[...] = got_ref[...]
        else:
            combine(got_ref, before_ref, before_out, count, width)

    @pl.when(jnp.logical_not(upper))
    def _():
        combine(total_ref, got_ref, total_out, count, width)
        if first:
            before_out[0:rows, :] = jnp.zeros((rows, LANES), F32)
            before_out[rows:, :] = jnp.ones((before_out.shape[0] - rows, LANES), F32)
        else:
            before_out[...] = before_ref[...]


def last_kernel(total_ref, got_ref, keep_ref, swap_ref, *refs, bit, first, count, width):
    before_ref, refs = (None, refs) if first else (refs[0], refs[1:])
    final_ref, own_ref, hand_ref, before_now = refs
    upper = rank_bit(bit) == 1
    odd = rank_bit(0) == 1
    rows = count * width

    @pl.when(upper)
    def _():
        combine(got_ref, total_ref, final_ref, count, width, decay=False)
        if first:
            before_now[...] = got_ref[0:rows, :]
        else:
            combine(got_ref, before_ref, before_now, count, width, decay=False)

    @pl.when(jnp.logical_not(upper))
    def _():
        combine(total_ref, got_ref, final_ref, count, width, decay=False)
        before_now[...] = jnp.zeros_like(before_now) if first else before_ref[0:rows, :]

    @pl.when(odd)
    def _():
        combine(before_now, swap_ref, own_ref, count, width, decay=False)
        hand_ref[...] = before_now[...]

    @pl.when(jnp.logical_not(odd))
    def _():
        own_ref[...] = before_now[...]
        combine(before_now, keep_ref, hand_ref, count, width, decay=False)


def output_kernel(*refs, parts, width):
    states, (queries_ref, grown_ref, inner_ref, *_, out_hbm, held, sent) = refs[: len(parts)], refs[len(parts) :]
    copies = []
    done = 0
    for k, ((kept, offset), state_ref) in enumerate(zip(parts, states, strict=True)):
        lanes = state_ref.shape[0]
        start = (half_start(kept, out_hbm.shape[1] // width) + offset) * width
        columns = pl.ds(pl.multiple_of(start, LANES), lanes)
        carried = lax.dot_general(queries_ref[...], state_ref[...].astype(BF16), NT, preferred_element_type=F32)
        held[:, done : done + lanes] = (inner_ref[:, columns] + carried * grown_ref[:, columns]).astype(BF16)
        copies.append(pltpu.make_async_copy(held.at[:, done : done + lanes], out_hbm.at[:, columns], sent.at[k]))
        copies[-1].start()
        done += lanes
    for copy in copies:
        copy.wait()


def pack_kernel(
    values_ref, decay_ref, keys_ref, score_ref, parent_ref, done_ref, length_ref, first_ref, out_ref, *, width
):
    steps, wide = values_ref.shape
    heads = decay_ref.shape[1]
    decays = spread(decay_ref[...], 0, heads, width)
    values = values_ref[...].astype(F32)
    lane = iota((1, LANES), 1)
    lines = wide // LANES
    for step in range(steps):
        row = jnp.zeros((1, LANES), F32)
        for k, ref in enumerate((score_ref, parent_ref, done_ref, length_ref, first_ref)):
            place = step if ref.shape[1] > 1 else 0
            row = jnp.where(lane == k, ref[0:1, place : place + 1].astype(F32), row)
        out_ref[step : step + 1, :] = row
        start = 2 * steps + step * 2 * lines
        for k in range(lines):
            lanes = slice(k * LANES, (k + 1) * LANES)
            out_ref[start + k : start + k + 1, :] = values[step : step + 1, lanes]
            out_ref[start + lines + k : start + lines + k + 1, :] = decays[step : step + 1, lanes]
    out_ref[steps : 2 * steps, :] = keys_ref[...].astype(F32)


def whole_kernel(final_ref, next_ref, far_ref, out_ref):
    home = lax.axis_index("seq") == lax.axis_index("beam")
    for half in range(HALVES):
        local = rank_bit(0) == half

        @pl.when(home & local)
        def _():
            out_ref[half] = final_ref[...]

        @pl.when(home ^ local)
        def _():
            out_ref[half] = next_ref[...]

        @pl.when(jnp.logical_not(home | local))
        def _():
            out_ref[half] = far_ref[...]


def either_kernel(mine_ref, got_ref, out_ref, *, bits):
    has = ((lax.axis_index("seq") ^ lax.axis_index("beam")) & bits) == 0

    @pl.when(has)
    def _():
        out_ref[...] = mine_ref[...]

    @pl.when(jnp.logical_not(has))
    def _():
        out_ref[...] = got_ref[...]


def lineage_kernel(
    rows_ref, queries_ref, grow_ref, part_ref, fresh_ref, shrink_ref, ranked_ref,
    outer_ref, key_ref, scores, counts, scalar_ref, arrived, *, slots, steps, wide, width
):
    (copy,) = fetch(arrived, (rows_ref.at[:, pl.ds(0, 2 * steps), :], scalar_ref))
    copy.wait()
    lines = wide // LANES
    flat = lambda x: jnp.concatenate([x[k : k + 1, :] for k in range(lines)], axis=1)
    me = lax.axis_index("beam")
    ranks_row = jnp.zeros((1, LANES), F32)
    done = lambda slot, step: scalar_ref[slot, step, 2]
    parent = lambda slot, step: scalar_ref[slot, step, 1].astype(jnp.int32)
    for slot in range(slots):
        scores[0, slot] = scalar_ref[slot, 0, 4]
        counts[0, slot] = scalar_ref[slot, 0, 3]
    lane = iota((1, LANES), 1)
    for step in range(steps):
        score_row = jnp.zeros((1, LANES), F32)
        count_row = jnp.zeros((1, LANES), F32)
        for slot in range(slots):
            source = parent(slot, step)
            live = 1.0 - done(slot, step)
            score = scores[step, source] + live * scalar_ref[slot, step, 0]
            tally = counts[step, source] + live
            scores[step + 1, slot] = score
            counts[step + 1, slot] = tally
            score_row = jnp.where(lane == slot, score, score_row)
            count_row = jnp.where(lane == slot, tally, count_row)
        normed = score_row * jnp.exp(-0.6 * jnp.log((5.0 + count_row) / 6.0))
        best = jnp.max(jnp.where(lane < slots, normed, -jnp.inf), axis=1, keepdims=True)
        mine = jnp.sum(jnp.where(lane == me, normed, 0.0), axis=1, keepdims=True)
        ranks_row = jnp.where(lane == step, mine - best, ranks_row)
    ranked_ref[...] = ranks_row[:, 0:steps]

    for ref in (grow_ref, part_ref, outer_ref, key_ref):
        ref[...] = jnp.zeros_like(ref)
    for step in range(steps):
        slot = me
        factor = jnp.ones((lines, LANES), F32)
        part = jnp.zeros((lines, LANES), F32)
        query = queries_ref[step : step + 1, :].astype(F32)
        live_now = 1.0 - done(me, step)
        for back in range(step, -1, -1):
            start = 2 * steps + back * 2 * lines
            live = 1.0 - done(slot, back)
            values = rows_ref[slot, start : start + lines, :]
            key = rows_ref[slot, steps + back : steps + back + 1, :]
            weight = factor * (values * live)
            part = part + weight * jnp.sum(key * query, axis=1, keepdims=True)
            if step == steps - 1:
                outer_ref[back : back + 1, :] = flat(weight)
                key_ref[back : back + 1, :] = key
            factor = factor * jnp.exp(rows_ref[slot, start + lines : start + 2 * lines, :] * live)
            slot = parent(slot, back)
        grow_ref[step : step + 1, :] = flat(factor * live_now)
        part_ref[step : step + 1, :] = flat(part * live_now)
        if step == steps - 1:
            keys = jnp.concatenate([key_ref[...].astype(BF16)] * 3, axis=0)
            fresh_ref[...] = lax.dot_general(thirds(outer_ref[...], 0), keys, TN, preferred_element_type=F32)
            count = shrink_ref.shape[0]
            pick = iota((count, wide), 1) == iota((count, wide), 0) * width
            shrink_ref[...] = jnp.broadcast_to(
                jnp.sum(jnp.where(pick, flat(factor), 0.0), axis=1, keepdims=True), (count, LANES)
            )


def decode_kernel(
    final_ref, queries_ref, grow_ref, part_ref, fresh_ref, shrink_ref, *refs, stretches, offset, count, width, last, given
):
    if given:
        earlier_ref, refs = refs[0], refs[2:]
    states_hbm, out_ref, held, sent = refs
    steps = queries_ref.shape[0]
    rows = count * width
    stretch = grow_ref.shape[1] // stretches
    copies = []
    for k in range(stretches):
        start = k * stretch + offset * width
        final = final_ref[k]
        product = lax.dot_general(queries_ref[...], final.astype(BF16), NT, preferred_element_type=F32)
        lanes = slice(start, start + rows)
        result = (grow_ref[0:steps, lanes] * product + part_ref[0:steps, lanes]).astype(BF16)
        if last:
            out_ref[:, lanes] = result
        else:
            out_ref[:, k * rows : (k + 1) * rows] = result
        for h in range(count):
            inside = slice(h * width, (h + 1) * width)
            head = start // width + h
            held[k, inside, :] = (
                shrink_ref[head : head + 1, :] * final[inside, :] + fresh_ref[start + h * width : start + (h + 1) * width, :]
            )
        copies.append(pltpu.make_async_copy(held.at[k], states_hbm.at[pl.ds(start, rows), :], sent.at[k]))
        copies[-1].start()
        if given:
            before = earlier_ref.shape[1] // stretches
            out_ref[:, k * stretch : k * stretch + before] = earlier_ref[:, k * before : (k + 1) * before]
    for copy in copies:
        copy.wait()


def emit_states(final, offset, count, width, lines, earlier, last):
    wide, steps = lines[1].shape[1], lines[0].shape[0]
    rows, stretches = count * width, final.shape[0]
    given = () if earlier is None else (earlier[1], earlier[0])
    return call(
        functools.partial(
            decode_kernel, stretches=stretches, offset=offset, count=count, width=width, last=last, given=bool(given)
        ),
        (final,) + lines + given,
        (
            jax.ShapeDtypeStruct((wide, LANES), F32),
            jax.ShapeDtypeStruct((steps, wide if last else stretches * rows), BF16),
        ),
        [VMEM] * 6 + [VMEM, HBM][: len(given)],
        out_specs=(HBM, VMEM),
        scratch_shapes=[pltpu.VMEM((stretches, rows, LANES), F32), pltpu.SemaphoreType.DMA((stretches,))],
        input_output_aliases={7: 0} if given else {},
    )


def on_device(
    prompt_values, prompt_keys, prompt_queries, logarithm_state_decay, step_values, step_keys, step_queries, step_decay,
    step_logprob, parents, finished, lengths, init_score, *, ranks, slots
):
    here = lambda x: pltpu.with_memory_space_constraint(x, pltpu.HBM)
    prompt_values, prompt_keys, prompt_queries = here(prompt_values), here(prompt_keys), here(prompt_queries)
    tokens, heads = logarithm_state_decay.shape
    width = prompt_values.shape[1] // heads
    steps = step_values.shape[0]
    wide = step_values.shape[2]
    own_heads = wide // width
    half_heads = heads // HALVES
    unit = LANES // width
    first_count = int(half_heads // unit * SHARE) * unit
    counts = (first_count, half_heads - first_count)
    offsets = (0, counts[0])
    array = lambda *shape, dtype=F32: jax.ShapeDtypeStruct(shape, dtype)
    messages = [array(count * width + -(-count // SUB) * SUB, LANES) for count in counts]
    levels = ranks.bit_length() - 1
    rank = lax.axis_index("seq")

    sums, turned, send_a = call(
        functools.partial(first_kernel, count=counts[0], width=width),
        (prompt_values, prompt_keys, here(logarithm_state_decay.T)),
        (array(tokens, heads), array(heads, tokens), messages[0]),
        [HBM] * 3,
        scratch_shapes=[
            pltpu.VMEM((tokens, counts[0] * width), BF16), pltpu.VMEM((tokens, LANES), BF16), pltpu.VMEM((heads, tokens), F32),
            pltpu.SemaphoreType.DMA((3,)),
        ],
    )
    swap = [(k, k ^ 1) for k in range(ranks)]
    got_a = permute(send_a, "seq", swap)

    def more_states(kept, offset, parts):
        return call(
            functools.partial(state_kernel, kept=kept, offset=offset, counts=[counts[sub] for sub in parts], width=width),
            (prompt_values, prompt_keys, sums),
            [messages[sub] for sub in parts],
            [HBM, HBM, VMEM],
            scratch_shapes=[
                pltpu.VMEM((tokens, sum(counts[sub] for sub in parts) * width), BF16), pltpu.VMEM((tokens, LANES), BF16),
                pltpu.SemaphoreType.DMA((2,)),
            ],
        )

    (send_b,) = more_states(False, offsets[1], (1,))
    got_b = permute(send_b, "seq", swap)
    keep_a, keep_b = more_states(True, 0, (0, 1))
    keeps, swaps = (keep_a, keep_b), (got_a, got_b)

    packed = call(
        functools.partial(pack_kernel, width=width),
        (
            step_values[:, 0], step_decay[:, 0], step_keys[:, 0], step_logprob.T, parents.T, finished.T, lengths[None],
            init_score[None],
        ),
        array(2 * steps * (1 + wide // LANES), LANES),
        [VMEM] * 8,
    )
    queries = step_queries[:, 0]

    *lines, ranked = call(
        functools.partial(lineage_kernel, slots=slots, steps=steps, wide=wide, width=width),
        (gather(packed).reshape(slots, -1, LANES), queries),
        (array(SUB, wide), array(SUB, wide), array(wide, LANES), array(own_heads, LANES), array(1, steps)),
        [VMEM, VMEM],
        scratch_shapes=[
            pltpu.VMEM((SUB, wide), F32), pltpu.VMEM((SUB, LANES), F32),
            pltpu.SMEM((steps + 1, slots), F32), pltpu.SMEM((steps + 1, slots), F32),
            pltpu.SMEM((slots, 2 * steps, LANES), F32), pltpu.SemaphoreType.DMA((1,)),
        ],
    )
    lines, ranked = (queries, *lines), ranked.reshape(steps, 1)

    inner, grown = call(
        functools.partial(inner_kernel, count=heads // INNER, width=width),
        (prompt_values, prompt_keys, prompt_queries, sums, turned),
        (array(tokens, heads * width),) * 2,
        [HBM, HBM, HBM, VMEM, VMEM],
        scratch_shapes=[
            pltpu.VMEM(prompt_values.shape, BF16), pltpu.VMEM((tokens, LANES), BF16), pltpu.VMEM((tokens, LANES), BF16),
            pltpu.VMEM((tokens, LANES), F32), pltpu.SemaphoreType.DMA((3,)),
        ],
        flops=100_000_000,
    )

    direct = ranks == slots
    states = step_out = None
    finals, owns, backs = [], [], []
    for sub, count in enumerate(counts):
        sizes = dict(count=count, width=width)
        rows, message = count * width, messages[sub]
        total = call(functools.partial(pair_kernel, **sizes), (keeps[sub], swaps[sub]), message, [VMEM] * 2)
        before = ()
        for level in range(1, levels):
            got = permute(total, "seq", [(k, k ^ (1 << level)) for k in range(ranks)])
            if level < levels - 1:
                before_now, total = call(
                    functools.partial(round_kernel, bit=level, first=level == 1, **sizes),
                    (total, got) + before,
                    (message, message),
                    [VMEM] * (2 + len(before)),
                )
                before = (before_now,)
        final, own, hand = call(
            functools.partial(last_kernel, bit=levels - 1, first=levels == 2, **sizes),
            (total, got, keeps[sub], swaps[sub]) + before,
            (array(rows, LANES),) * 3,
            [VMEM] * (4 + len(before)),
            scratch_shapes=[pltpu.VMEM((rows, LANES), F32)],
        )
        finals.append(final)
        if direct:
            far = slots // HALVES
            near = [((g ^ 1) * slots + g, g * slots + g) for g in range(ranks)]
            near += [(g * slots + g, g * slots + (g ^ far)) for g in range(ranks)]
            came = permute(final, ("seq", "beam"), near)
            if sub == 0:
                across = permute(came, ("seq", "beam"), [(g * slots + g, g * slots + (g ^ far)) for g in range(ranks)])
            else:
                across = permute(final, ("seq", "beam"), [((g ^ 1) * slots + g, g * slots + (g ^ far)) for g in range(ranks)])
            full = call(whole_kernel, (final, came, across), array(HALVES, rows, LANES), [VMEM] * 3)
            bit = 1
            while bit < far:
                have = [b for b in range(slots) if b & (far - 1) < bit]
                pairs = [(g * slots + (g ^ b), g * slots + (g ^ b ^ bit)) for g in range(ranks) for b in have]
                handed = permute(full, ("seq", "beam"), pairs)
                full = call(
                    functools.partial(either_kernel, bits=bit), (full, handed), array(HALVES, rows, LANES),
                    [VMEM] * 2,
                )
                bit *= 2
        back = permute(hand, "seq", [(k, k ^ 1) for k in range(1, ranks) if k != 1] + [(0, 1)])
        if direct:
            states, step_out = emit_states(
                full, offsets[sub], count, width, lines, (states, step_out) if sub else None, sub == 1
            )
        owns.append(own)
        backs.append(back)

    def outputs(states, parts, given):
        lanes = sum(state.shape[0] for state in states)
        return call(
            functools.partial(output_kernel, parts=parts, width=width),
            (*states, prompt_queries, grown, inner) + given,
            array(tokens, heads * width, dtype=BF16),
            [VMEM] * (len(states) + 3) + [HBM] * len(given),
            out_specs=HBM,
            scratch_shapes=[pltpu.VMEM((tokens, lanes), BF16), pltpu.SemaphoreType.DMA((len(states),))],
            input_output_aliases={len(states) + 3: 0} if given else {},
        )

    out = outputs((*owns, backs[0]), ((True, offsets[0]), (True, offsets[1]), (False, offsets[0])), ())
    out = outputs((backs[1],), ((False, offsets[1]),), (out,))
    if not direct:
        half = jnp.concatenate(finals)
        other = lax.ppermute(half, "seq", swap)
        odd = rank_bit(0) == 1
        both = jnp.concatenate([jnp.where(odd, other, half), jnp.where(odd, half, other)])
        every = gather(both)
        full = lax.dynamic_slice_in_dim(every, rank * wide, wide, 0)[None]
        states, step_out = emit_states(full, 0, own_heads, width, lines, None, True)
    return out, step_out.reshape(steps, 1, wide), ranked, states.reshape(1, wide, LANES)


def solution(mesh):
    ranks, slots = mesh.shape["seq"], mesh.shape["beam"]

    def body(*args):
        return on_device(*args, ranks=ranks, slots=slots)

    return jax.shard_map(
        body,
        mesh=mesh,
        in_specs=(
            P(("groups", "seq"), "beam"),
            P(("groups", "seq"), None),
            P(("groups", "seq"), None),
            P(("groups", "seq"), "beam"),
            P("groups", "beam", "seq"),
            P("groups", "beam", None),
            P("groups", "beam", None),
            P("groups", "beam", "seq"),
            P("groups", "beam"),
            P("groups", "beam"),
            P("groups", "beam"),
            P(("groups", "beam")),
            P(("groups", "beam")),
        ),
        out_specs=(
            P(("groups", "seq"), "beam"),
            P("groups", "beam", "seq"),
            P("groups", "beam"),
            P(("groups", "beam"), "seq", None),
        ),
        check_vma=False,
    )
```

```python
import functools

import jax
import jax.numpy as jnp
from jax import lax
from jax.experimental import pallas as pl
from jax.experimental.pallas import tpu as pltpu
from jax.sharding import PartitionSpec as P


LANES = 128
SUB = 8
HALVES = 2
SHARE = 3 / 8
INNER = 4
F32 = jnp.float32
BF16 = jnp.bfloat16
TN = (((0,), (0,)), ((), ()))
NT = (((1,), (1,)), ((), ()))

VMEM = pl.BlockSpec(memory_space=pltpu.VMEM)
HBM = pl.BlockSpec(memory_space=pltpu.HBM)
SMEM = pl.BlockSpec(memory_space=pltpu.SMEM)


def call(body, args, out_shape, in_specs=None, flops=1_000_000, **kwargs):
    return pl.pallas_call(
        body,
        out_shape=out_shape,
        in_specs=in_specs,
        cost_estimate=pl.CostEstimate(flops=flops, bytes_accessed=1_000_000, transcendentals=0),
        compiler_params=pltpu.CompilerParams(vmem_limit_bytes=8 * 2**20),
        **kwargs,
    )(*args)


def permute(array, axis, pairs):
    return lax.ppermute(array, axis, pairs)


def gather(array):
    return lax.all_gather(array, "beam", axis=0, tiled=True)


def iota(shape, axis):
    return lax.broadcasted_iota(jnp.int32, shape, axis)


def head_lanes(heads, first, count, width):
    shape = (heads, count * width)
    return (iota(shape, 0) == first + iota(shape, 1) // width).astype(F32)


def thirds(x, axis):
    high = x.astype(BF16)
    rest = x - high.astype(F32)
    middle = rest.astype(BF16)
    return jnp.concatenate([high, middle, (rest - middle.astype(F32)).astype(BF16)], axis=axis)


def spread(x, first, count, width):
    hot = head_lanes(x.shape[1], first, count, width).astype(BF16)
    return jnp.dot(thirds(x, 1), jnp.concatenate([hot] * 3, axis=0), preferred_element_type=F32)


def part_state(values, keys, sums, first, count, width, out_ref):
    heads = sums.shape[1]
    last = sums[-1:, :]
    scaled = (values.astype(F32) * spread(jnp.exp(last - sums), first, count, width)).astype(BF16)
    rows = count * width
    out_ref[0:rows, :] = lax.dot_general(scaled, keys, TN, preferred_element_type=F32)
    pad = out_ref.shape[0] - rows
    pick = iota((pad, heads), 1) == first + iota((pad, heads), 0)
    total = jnp.sum(jnp.where(pick, last, 0.0), axis=1, keepdims=True)
    out_ref[rows:, :] = jnp.broadcast_to(jnp.exp(total), (pad, LANES))


def rank_bit(k):
    return (lax.axis_index("seq") >> k) & 1


def half_start(kept, heads):
    return (rank_bit(0) if kept else rank_bit(0) ^ 1) * (heads // HALVES)


def fetch(arrived, *pairs):
    copies = [pltpu.make_async_copy(source, target, arrived.at[k]) for k, (source, target) in enumerate(pairs)]
    for copy in copies:
        copy.start()
    return copies


def first_kernel(values_hbm, keys_hbm, decay_hbm, sums_ref, turned_ref, out_ref, values, keys, decay, arrived, *, count, width):
    heads, tokens = decay.shape
    start = half_start(False, heads)
    columns = values_hbm.at[:, pl.ds(pl.multiple_of(start * width, LANES), count * width)]
    copies = fetch(arrived, (decay_hbm, decay), (columns, values), (keys_hbm, keys))
    copies[0].wait()
    upper = (iota((tokens, tokens), 0) <= iota((tokens, tokens), 1)).astype(F32).astype(BF16)
    terms = jnp.dot(thirds(decay[...], 0), upper, preferred_element_type=F32)
    turned = terms[0:heads] + (terms[heads : 2 * heads] + terms[2 * heads :])
    turned_ref[...] = turned
    sums = turned.T
    sums_ref[...] = sums
    for copy in copies[1:]:
        copy.wait()
    part_state(values[...], keys[...], sums, start, count, width, out_ref)


def state_kernel(values_hbm, keys_hbm, sums_ref, *refs, kept, offset, counts, width):
    *out_refs, values_ref, keys_ref, arrived = refs
    start = half_start(kept, sums_ref.shape[1]) + offset
    columns = pl.ds(pl.multiple_of(start * width, LANES), sum(counts) * width)
    for copy in fetch(arrived, (values_hbm.at[:, columns], values_ref), (keys_hbm, keys_ref)):
        copy.wait()
    done = 0
    for count, out_ref in zip(counts, out_refs, strict=True):
        values = values_ref[:, done * width : (done + count) * width]
        part_state(values, keys_ref[...], sums_ref[...], start + done, count, width, out_ref)
        done += count


def inner_kernel(
    values_hbm, keys_hbm, queries_hbm, sums_ref, turned_ref, out_ref, grown_ref,
    values_ref, keys_ref, queries_ref, wide_ref, arrived, *, count, width
):
    copies = fetch(arrived, (keys_hbm, keys_ref), (queries_hbm, queries_ref), (values_hbm, values_ref))
    tokens, heads = sums_ref.shape
    half = tokens // 2
    wide_ref[...] = jnp.zeros_like(wide_ref)
    wide_ref[:, 0:heads] = sums_ref[...]
    for copy in copies:
        copy.wait()
    scores = lax.dot_general(queries_ref[...], keys_ref[...], NT, preferred_element_type=F32)
    lower = iota((half, half), 0) >= iota((half, half), 1)
    top = jnp.where(lower, scores[:half, :half], 0.0)
    left = scores[half:, :half]
    bottom = jnp.where(lower, scores[half:, half:], 0.0)
    per_store = LANES // width
    lane = iota((tokens, LANES), 1) // width

    def group(g, carry):
        wide = pltpu.roll(wide_ref[...], lax.rem(LANES - g * count, LANES), 1)
        for k in range(count // per_store):
            place = pl.ds(pl.multiple_of((g * count + k * per_store) * width, LANES), LANES)
            values = values_ref[:, place]
            tops, bottoms = [], []
            grown = wide[:, k * per_store : k * per_store + 1]
            for m in range(1, per_store):
                grown = jnp.where(lane == m, wide[:, k * per_store + m : k * per_store + m + 1], grown)
            grown_ref[:, place] = jnp.exp(jnp.broadcast_to(grown, (tokens, LANES)))
            for m in range(per_store):
                h = k * per_store + m
                column = wide[:, h : h + 1]
                row = turned_ref[pl.ds(g * count + h, 1), :]
                x = values[:, m * width : (m + 1) * width]
                w0 = (top * jnp.exp(jnp.minimum(column[:half] - row[:, :half], 0.0))).astype(BF16)
                w1 = (left * jnp.exp(column[half:] - row[:, :half])).astype(BF16)
                w2 = (bottom * jnp.exp(jnp.minimum(column[half:] - row[:, half:], 0.0))).astype(BF16)
                tops.append(jnp.dot(w0, x[:half], preferred_element_type=F32))
                bottoms.append(jnp.dot(jnp.concatenate([w1, w2], axis=1), x, preferred_element_type=F32))
            out_ref[0:half, place] = jnp.concatenate(tops, axis=1)
            out_ref[half:, place] = jnp.concatenate(bottoms, axis=1)
        return carry

    lax.fori_loop(0, heads // count, group, 0)


def combine(low, high, out, count, width, decay=True):
    rows = count * width
    for h in range(count):
        place = slice(h * width, (h + 1) * width)
        out[place, :] = high[rows + h : rows + h + 1, :] * low[place, :] + high[place, :]
    if decay:
        out[rows:, :] = low[rows:, :] * high[rows:, :]


def pair_kernel(keep_ref, got_ref, out_ref, *, count, width):
    odd = rank_bit(0) == 1

    @pl.when(odd)
    def _():
        combine(got_ref, keep_ref, out_ref, count, width)

    @pl.when(jnp.logical_not(odd))
    def _():
        combine(keep_ref, got_ref, out_ref, count, width)


def round_kernel(total_ref, got_ref, *refs, bit, first, count, width):
    before_ref, refs = (None, refs) if first else (refs[0], refs[1:])
    before_out, total_out = refs
    upper = rank_bit(bit) == 1
    rows = count * width

    @pl.when(upper)
    def _():
        combine(got_ref, total_ref, total_out, count, width)
        if first:
            before_out[...] = got_ref[...]
        else:
            combine(got_ref, before_ref, before_out, count, width)

    @pl.when(jnp.logical_not(upper))
    def _():
        combine(total_ref, got_ref, total_out, count, width)
        if first:
            before_out[0:rows, :] = jnp.zeros((rows, LANES), F32)
            before_out[rows:, :] = jnp.ones((before_out.shape[0] - rows, LANES), F32)
        else:
            before_out[...] = before_ref[...]


def last_kernel(total_ref, got_ref, keep_ref, swap_ref, *refs, bit, first, count, width):
    before_ref, refs = (None, refs) if first else (refs[0], refs[1:])
    final_ref, own_ref, hand_ref, before_now = refs
    upper = rank_bit(bit) == 1
    odd = rank_bit(0) == 1
    rows = count * width

    @pl.when(upper)
    def _():
        combine(got_ref, total_ref, final_ref, count, width, decay=False)
        if first:
            before_now[...] = got_ref[0:rows, :]
        else:
            combine(got_ref, before_ref, before_now, count, width, decay=False)

    @pl.when(jnp.logical_not(upper))
    def _():
        combine(total_ref, got_ref, final_ref, count, width, decay=False)
        before_now[...] = jnp.zeros_like(before_now) if first else before_ref[0:rows, :]

    @pl.when(odd)
    def _():
        combine(before_now, swap_ref, own_ref, count, width, decay=False)
        hand_ref[...] = before_now[...]

    @pl.when(jnp.logical_not(odd))
    def _():
        own_ref[...] = before_now[...]
        combine(before_now, keep_ref, hand_ref, count, width, decay=False)


def output_kernel(*refs, parts, width):
    states, (queries_ref, grown_ref, inner_ref, *_, out_hbm, held, sent) = refs[: len(parts)], refs[len(parts) :]
    copies = []
    done = 0
    for (kept, offset), state_ref in zip(parts, states, strict=True):
        base = half_start(kept, out_hbm.shape[1] // width) * width
        cut = state_ref.shape[0] // 2 // LANES * LANES
        for first, lanes in ((0, cut), (cut, state_ref.shape[0] - cut)):
            if lanes == 0:
                continue
            columns = pl.ds(pl.multiple_of(base + offset * width + first, LANES), lanes)
            state = state_ref[first : first + lanes, :].astype(BF16)
            carried = lax.dot_general(queries_ref[...], state, NT, preferred_element_type=F32)
            held[:, done : done + lanes] = (inner_ref[:, columns] + carried * grown_ref[:, columns]).astype(BF16)
            copies.append(
                pltpu.make_async_copy(held.at[:, done : done + lanes], out_hbm.at[:, columns], sent.at[len(copies)])
            )
            copies[-1].start()
            done += lanes
    for copy in copies:
        copy.wait()


def pack_kernel(
    values_ref, decay_ref, keys_ref, score_ref, parent_ref, done_ref, length_ref, first_ref, out_ref, *, width
):
    steps, wide = values_ref.shape
    heads = decay_ref.shape[1]
    decays = spread(decay_ref[...], 0, heads, width)
    values = values_ref[...].astype(F32)
    lane = iota((1, LANES), 1)
    lines = wide // LANES
    for step in range(steps):
        row = jnp.zeros((1, LANES), F32)
        for k, ref in enumerate((score_ref, parent_ref, done_ref, length_ref, first_ref)):
            place = step if ref.shape[1] > 1 else 0
            row = jnp.where(lane == k, ref[0:1, place : place + 1].astype(F32), row)
        out_ref[step : step + 1, :] = row
        start = 2 * steps + step * 2 * lines
        for k in range(lines):
            lanes = slice(k * LANES, (k + 1) * LANES)
            out_ref[start + k : start + k + 1, :] = values[step : step + 1, lanes]
            out_ref[start + lines + k : start + lines + k + 1, :] = decays[step : step + 1, lanes]
    out_ref[steps : 2 * steps, :] = keys_ref[...].astype(F32)


def whole_kernel(final_ref, next_ref, far_ref, out_ref):
    home = lax.axis_index("seq") == lax.axis_index("beam")
    for half in range(HALVES):
        local = rank_bit(0) == half

        @pl.when(home & local)
        def _():
            out_ref[half] = final_ref[...]

        @pl.when(home ^ local)
        def _():
            out_ref[half] = next_ref[...]

        @pl.when(jnp.logical_not(home | local))
        def _():
            out_ref[half] = far_ref[...]


def either_kernel(mine_ref, got_ref, out_ref, *, bits):
    has = ((lax.axis_index("seq") ^ lax.axis_index("beam")) & bits) == 0

    @pl.when(has)
    def _():
        out_ref[...] = mine_ref[...]

    @pl.when(jnp.logical_not(has))
    def _():
        out_ref[...] = got_ref[...]


def stack_kernel(*refs):
    *parts, out_ref = refs
    done = 0
    for part in parts:
        out_ref[done : done + part.shape[0]] = part[...]
        done += part.shape[0]


def lineage_kernel(*refs, offsets, slots, steps, wide, width):
    blocks, refs = refs[: len(offsets)], refs[len(offsets) :]
    queries_ref, grow_ref, part_ref, fresh_ref, shrink_ref, ranked_ref = refs[:6]
    outer_ref, key_ref, scores, counts, scalar_ref, rows_ref, arrived = refs[6:]
    places = [(block, k, away) for block, some in zip(blocks, offsets, strict=True) for k, away in enumerate(some)]
    copies = fetch(arrived, *((block.at[k, pl.ds(0, 2 * steps), :], scalar_ref.at[away]) for block, k, away in places))
    for block, k, away in places:
        rows_ref[away] = block[k]
    for copy in copies:
        copy.wait()
    lines = wide // LANES
    flat = lambda x: jnp.concatenate([x[k : k + 1, :] for k in range(lines)], axis=1)
    me = lax.axis_index("beam")
    ranks_row = jnp.zeros((1, LANES), F32)
    done = lambda slot, step: scalar_ref[slot ^ me, step, 2]
    parent = lambda slot, step: scalar_ref[slot ^ me, step, 1].astype(jnp.int32)
    for slot in range(slots):
        scores[0, slot] = scalar_ref[slot ^ me, 0, 4]
        counts[0, slot] = scalar_ref[slot ^ me, 0, 3]
    lane = iota((1, LANES), 1)
    for step in range(steps):
        score_row = jnp.zeros((1, LANES), F32)
        count_row = jnp.zeros((1, LANES), F32)
        for slot in range(slots):
            source = parent(slot, step)
            live = 1.0 - done(slot, step)
            score = scores[step, source] + live * scalar_ref[slot ^ me, step, 0]
            tally = counts[step, source] + live
            scores[step + 1, slot] = score
            counts[step + 1, slot] = tally
            score_row = jnp.where(lane == slot, score, score_row)
            count_row = jnp.where(lane == slot, tally, count_row)
        normed = score_row * jnp.exp(-0.6 * jnp.log((5.0 + count_row) / 6.0))
        best = jnp.max(jnp.where(lane < slots, normed, -jnp.inf), axis=1, keepdims=True)
        mine = jnp.sum(jnp.where(lane == me, normed, 0.0), axis=1, keepdims=True)
        ranks_row = jnp.where(lane == step, mine - best, ranks_row)
    ranked_ref[...] = ranks_row[:, 0:steps]

    for ref in (grow_ref, part_ref, outer_ref, key_ref):
        ref[...] = jnp.zeros_like(ref)
    for step in range(steps):
        slot = me
        factor = jnp.ones((lines, LANES), F32)
        part = jnp.zeros((lines, LANES), F32)
        query = queries_ref[step : step + 1, :].astype(F32)
        live_now = 1.0 - done(me, step)
        for back in range(step, -1, -1):
            start = 2 * steps + back * 2 * lines
            live = 1.0 - done(slot, back)
            values = rows_ref[slot ^ me, start : start + lines, :]
            key = rows_ref[slot ^ me, steps + back : steps + back + 1, :]
            weight = factor * (values * live)
            part = part + weight * jnp.sum(key * query, axis=1, keepdims=True)
            if step == steps - 1:
                outer_ref[back : back + 1, :] = flat(weight)
                key_ref[back : back + 1, :] = key
            factor = factor * jnp.exp(rows_ref[slot ^ me, start + lines : start + 2 * lines, :] * live)
            slot = parent(slot, back)
        grow_ref[step : step + 1, :] = flat(factor * live_now)
        part_ref[step : step + 1, :] = flat(part * live_now)
        if step == steps - 1:
            keys = jnp.concatenate([key_ref[...].astype(BF16)] * 3, axis=0)
            fresh_ref[...] = lax.dot_general(thirds(outer_ref[...], 0), keys, TN, preferred_element_type=F32)
            count = shrink_ref.shape[0]
            pick = iota((count, wide), 1) == iota((count, wide), 0) * width
            shrink_ref[...] = jnp.broadcast_to(
                jnp.sum(jnp.where(pick, flat(factor), 0.0), axis=1, keepdims=True), (count, LANES)
            )


def decode_kernel(
    final_ref, queries_ref, grow_ref, part_ref, fresh_ref, shrink_ref, *refs, stretches, offset, count, width, last, given
):
    if given:
        earlier_ref, refs = refs[0], refs[2:]
    states_hbm, out_ref, held, sent = refs
    steps = queries_ref.shape[0]
    rows = count * width
    stretch = grow_ref.shape[1] // stretches
    copies = []
    for k in range(stretches):
        start = k * stretch + offset * width
        for h in range(count):
            inside = slice(h * width, (h + 1) * width)
            head = start // width + h
            held[k, inside, :] = (
                shrink_ref[head : head + 1, :] * final_ref[k, inside, :]
                + fresh_ref[start + h * width : start + (h + 1) * width, :]
            )
        copies.append(pltpu.make_async_copy(held.at[k], states_hbm.at[pl.ds(start, rows), :], sent.at[k]))
        copies[-1].start()
    for k in range(stretches):
        start = k * stretch + offset * width
        product = lax.dot_general(queries_ref[...], final_ref[k].astype(BF16), NT, preferred_element_type=F32)
        lanes = slice(start, start + rows)
        result = (grow_ref[0:steps, lanes] * product + part_ref[0:steps, lanes]).astype(BF16)
        if last:
            out_ref[:, lanes] = result
        else:
            out_ref[:, k * rows : (k + 1) * rows] = result
        if given:
            before = earlier_ref.shape[1] // stretches
            out_ref[:, k * stretch : k * stretch + before] = earlier_ref[:, k * before : (k + 1) * before]
    for copy in copies:
        copy.wait()


def emit_states(final, offset, count, width, lines, earlier, last):
    wide, steps = lines[1].shape[1], lines[0].shape[0]
    rows, stretches = count * width, final.shape[0]
    given = () if earlier is None else (earlier[1], earlier[0])
    return call(
        functools.partial(
            decode_kernel, stretches=stretches, offset=offset, count=count, width=width, last=last, given=bool(given)
        ),
        (final,) + lines + given,
        (
            jax.ShapeDtypeStruct((wide, LANES), F32),
            jax.ShapeDtypeStruct((steps, wide if last else stretches * rows), BF16),
        ),
        [VMEM] * 6 + [VMEM, HBM][: len(given)],
        out_specs=(HBM, VMEM),
        scratch_shapes=[pltpu.VMEM((stretches, rows, LANES), F32), pltpu.SemaphoreType.DMA((stretches,))],
        input_output_aliases={7: 0} if given else {},
    )


def on_device(
    prompt_values, prompt_keys, prompt_queries, logarithm_state_decay, step_values, step_keys, step_queries, step_decay,
    step_logprob, parents, finished, lengths, init_score, *, ranks, slots
):
    here = lambda x: pltpu.with_memory_space_constraint(x, pltpu.HBM)
    prompt_values, prompt_keys, prompt_queries = here(prompt_values), here(prompt_keys), here(prompt_queries)
    tokens, heads = logarithm_state_decay.shape
    width = prompt_values.shape[1] // heads
    steps = step_values.shape[0]
    wide = step_values.shape[2]
    own_heads = wide // width
    half_heads = heads // HALVES
    unit = LANES // width
    first_count = int(half_heads // unit * SHARE) * unit
    counts = (first_count, half_heads - first_count)
    starts = (0, counts[0])
    array = lambda *shape, dtype=F32: jax.ShapeDtypeStruct(shape, dtype)
    messages = [array(count * width + -(-count // SUB) * SUB, LANES) for count in counts]
    levels = ranks.bit_length() - 1
    rank = lax.axis_index("seq")

    sums, turned, send_a = call(
        functools.partial(first_kernel, count=counts[0], width=width),
        (prompt_values, prompt_keys, here(logarithm_state_decay.T)),
        (array(tokens, heads), array(heads, tokens), messages[0]),
        [HBM] * 3,
        scratch_shapes=[
            pltpu.VMEM((tokens, counts[0] * width), BF16), pltpu.VMEM((tokens, LANES), BF16), pltpu.VMEM((heads, tokens), F32),
            pltpu.SemaphoreType.DMA((3,)),
        ],
    )
    swap = [(k, k ^ 1) for k in range(ranks)]
    got_a = permute(send_a, "seq", swap)

    def more_states(kept, offset, parts):
        return call(
            functools.partial(state_kernel, kept=kept, offset=offset, counts=[counts[sub] for sub in parts], width=width),
            (prompt_values, prompt_keys, sums),
            [messages[sub] for sub in parts],
            [HBM, HBM, VMEM],
            scratch_shapes=[
                pltpu.VMEM((tokens, sum(counts[sub] for sub in parts) * width), BF16), pltpu.VMEM((tokens, LANES), BF16),
                pltpu.SemaphoreType.DMA((2,)),
            ],
        )

    (send_b,) = more_states(False, starts[1], (1,))
    got_b = permute(send_b, "seq", swap)
    keep_a, keep_b = more_states(True, 0, (0, 1))
    keeps, swaps = (keep_a, keep_b), (got_a, got_b)

    packed = call(
        functools.partial(pack_kernel, width=width),
        (
            step_values[:, 0], step_decay[:, 0], step_keys[:, 0], step_logprob.T, parents.T, finished.T, lengths[None],
            init_score[None],
        ),
        array(2 * steps * (1 + wide // LANES), LANES),
        [VMEM] * 8,
    )
    queries = step_queries[:, 0]

    blocks, offsets, bit = [packed[None]], [[0]], slots // 2
    while bit:
        if len(blocks) == 1:
            have = blocks[0]
        else:
            have = call(
                stack_kernel, blocks, array(sum(len(some) for some in offsets), *packed.shape),
                [VMEM] * len(blocks),
            )
        blocks.append(permute(have, "beam", [(b, b ^ bit) for b in range(slots)]))
        offsets.append([away ^ bit for some in offsets for away in some])
        bit //= 2
    *lines, ranked = call(
        functools.partial(lineage_kernel, offsets=offsets, slots=slots, steps=steps, wide=wide, width=width),
        (*blocks, queries),
        (array(SUB, wide), array(SUB, wide), array(wide, LANES), array(own_heads, LANES), array(1, steps)),
        [VMEM] * (len(blocks) + 1),
        scratch_shapes=[
            pltpu.VMEM((SUB, wide), F32), pltpu.VMEM((SUB, LANES), F32),
            pltpu.SMEM((steps + 1, slots), F32), pltpu.SMEM((steps + 1, slots), F32),
            pltpu.SMEM((slots, 2 * steps, LANES), F32), pltpu.VMEM((slots, *packed.shape), F32),
            pltpu.SemaphoreType.DMA((slots,)),
        ],
    )
    lines, ranked = (queries, *lines), ranked.reshape(steps, 1)

    inner, grown = call(
        functools.partial(inner_kernel, count=heads // INNER, width=width),
        (prompt_values, prompt_keys, prompt_queries, sums, turned),
        (array(tokens, heads * width),) * 2,
        [HBM, HBM, HBM, VMEM, VMEM],
        scratch_shapes=[
            pltpu.VMEM(prompt_values.shape, BF16), pltpu.VMEM((tokens, LANES), BF16), pltpu.VMEM((tokens, LANES), BF16),
            pltpu.VMEM((tokens, LANES), F32), pltpu.SemaphoreType.DMA((3,)),
        ],
        flops=100_000_000,
    )

    direct = ranks == slots
    states = step_out = None
    finals, owns, backs = [], [], []
    for sub, count in enumerate(counts):
        sizes = dict(count=count, width=width)
        rows, message = count * width, messages[sub]
        total = call(functools.partial(pair_kernel, **sizes), (keeps[sub], swaps[sub]), message, [VMEM] * 2)
        before = ()
        for level in range(1, levels):
            got = permute(total, "seq", [(k, k ^ (1 << level)) for k in range(ranks)])
            if level < levels - 1:
                before_now, total = call(
                    functools.partial(round_kernel, bit=level, first=level == 1, **sizes),
                    (total, got) + before,
                    (message, message),
                    [VMEM] * (2 + len(before)),
                )
                before = (before_now,)
        final, own, hand = call(
            functools.partial(last_kernel, bit=levels - 1, first=levels == 2, **sizes),
            (total, got, keeps[sub], swaps[sub]) + before,
            (array(rows, LANES),) * 3,
            [VMEM] * (4 + len(before)),
            scratch_shapes=[pltpu.VMEM((rows, LANES), F32)],
        )
        finals.append(final)
        if direct:
            far = slots // HALVES
            near = [((g ^ 1) * slots + g, g * slots + g) for g in range(ranks)]
            near += [(g * slots + g, g * slots + (g ^ far)) for g in range(ranks)]
            came = permute(final, ("seq", "beam"), near)
            if sub == 0:
                across = permute(came, ("seq", "beam"), [(g * slots + g, g * slots + (g ^ far)) for g in range(ranks)])
            else:
                across = permute(final, ("seq", "beam"), [((g ^ 1) * slots + g, g * slots + (g ^ far)) for g in range(ranks)])
            full = call(whole_kernel, (final, came, across), array(HALVES, rows, LANES), [VMEM] * 3)
            bit = 1
            while bit < far:
                have = [b for b in range(slots) if b & (far - 1) < bit]
                pairs = [(g * slots + (g ^ b), g * slots + (g ^ b ^ bit)) for g in range(ranks) for b in have]
                handed = permute(full, ("seq", "beam"), pairs)
                full = call(
                    functools.partial(either_kernel, bits=bit), (full, handed), array(HALVES, rows, LANES),
                    [VMEM] * 2,
                )
                bit *= 2
        back = permute(hand, "seq", [(k, k ^ 1) for k in range(1, ranks) if k != 1] + [(0, 1)])
        if direct:
            states, step_out = emit_states(
                full, starts[sub], count, width, lines, (states, step_out) if sub else None, sub == 1
            )
        owns.append(own)
        backs.append(back)

    def outputs(states, parts, given):
        lanes = sum(state.shape[0] for state in states)
        return call(
            functools.partial(output_kernel, parts=parts, width=width),
            (*states, prompt_queries, grown, inner) + given,
            array(tokens, heads * width, dtype=BF16),
            [VMEM] * (len(states) + 3) + [HBM] * len(given),
            out_specs=HBM,
            scratch_shapes=[pltpu.VMEM((tokens, lanes), BF16), pltpu.SemaphoreType.DMA((2 * len(states),))],
            input_output_aliases={len(states) + 3: 0} if given else {},
        )

    out = outputs((owns[0], backs[0]), ((True, starts[0]), (False, starts[0])), ())
    out = outputs((owns[1],), ((True, starts[1]),), (out,))
    out = outputs((backs[1],), ((False, starts[1]),), (out,))
    if not direct:
        half = jnp.concatenate(finals)
        other = lax.ppermute(half, "seq", swap)
        odd = rank_bit(0) == 1
        both = jnp.concatenate([jnp.where(odd, other, half), jnp.where(odd, half, other)])
        every = gather(both)
        full = lax.dynamic_slice_in_dim(every, rank * wide, wide, 0)[None]
        states, step_out = emit_states(full, 0, own_heads, width, lines, None, True)
    return out, step_out.reshape(steps, 1, wide), ranked, states.reshape(1, wide, LANES)


def solution(mesh):
    ranks, slots = mesh.shape["seq"], mesh.shape["beam"]

    def body(*args):
        return on_device(*args, ranks=ranks, slots=slots)

    step = jax.shard_map(
        body,
        mesh=mesh,
        in_specs=(
            P(("groups", "seq"), "beam"),
            P(("groups", "seq"), None),
            P(("groups", "seq"), None),
            P(("groups", "seq"), "beam"),
            P("groups", "beam", "seq"),
            P("groups", "beam", None),
            P("groups", "beam", None),
            P("groups", "beam", "seq"),
            P("groups", "beam"),
            P("groups", "beam"),
            P("groups", "beam"),
            P(("groups", "beam")),
            P(("groups", "beam")),
        ),
        out_specs=(
            P(("groups", "seq"), "beam"),
            P("groups", "beam", "seq"),
            P("groups", "beam"),
            P(("groups", "beam"), "seq", None),
        ),
        check_vma=False,
    )
    return step if ranks == slots else step
```
